32 devices in a mesh: north: 8 (over y, x, core), deep: 4 (over z).
Axes of the slice: x: 2, y: 2, z: 4, core: 2. Of those that a mesh axis runs over, the one named last changes fastest.
Arguments:
- velocity: float32 [4, 128, 64, 256], P(None, None, 'north', 'deep'), may hold values from -6 to 6
- coupling: float32 [4, 4], replicated, may hold values from -4 to 4
- symbol_x: float32 [128], replicated, may hold values from 0.3 to 3
- symbol_y: float32 [64], replicated, may hold values from 0.3 to 3
- symbol_z: float32 [256], replicated, may hold values from 0.3 to 3
Outputs:
- spectrum: float32 [4, 128, 64, 256], P(None, 'north', 'deep')
The draws below stay inside these ranges and needn't reach their ends.
All inputs are finite; a program needn't handle non-finite values.
Results may differ from the reference program's by a relative error of at most 0.00007.
Values sent between devices are 32-bit elements; how exact they have to be, the bound alone decides.
A program may use at most 128 MiB of HBM per device.

```python
import jax
import jax.numpy as jnp
from jax import lax

GRID_X = 128
GRID_Y = 64
GRID_Z = 256
FIELDS = 4


def steps_of(rng, dims, pieces, least, top_value):
    loudness = 1.0
    for position, shards_of in pieces:
        steps = jax.random.uniform(jax.random.fold_in(jax.random.fold_in(rng, 6), position), (shards_of,), jnp.float32, least / len(pieces), top_value / len(pieces))
        loudness = loudness * jnp.repeat(jnp.exp(steps), dims[position] // shards_of).reshape((-1,) + (1,) * (len(dims) - 1 - position))
    return loudness


def normal_values(key, shape, deviation, limit, pieces=(), kind=jnp.bfloat16):
    array = jax.random.normal(key, shape, jnp.float32) * deviation
    if len(pieces) > 0:
        array = steps_of(key, shape, pieces, -0.22, 0.18) * array
    return jnp.clip(array, min=-limit, max=limit).astype(kind)


def setup_inputs(seed: int = 0) -> dict:
    key_list = jax.random.split(jax.random.key(seed), 6)
    velocity = normal_values(key_list[0], (FIELDS, GRID_X, GRID_Y, GRID_Z), 1.0, 6.0, ((2, 8), (3, 4)), jnp.float32)
    coupling = normal_values(key_list[1], (FIELDS, FIELDS), 0.7, 4.0, (), jnp.float32)
    symbol_x = jnp.clip(jax.random.uniform(key_list[2], (GRID_X,), jnp.float32, 0.3, 3.0), 0.3, 3.0)
    symbol_y = jnp.clip(jax.random.uniform(key_list[3], (GRID_Y,), jnp.float32, 0.3, 3.0), 0.3, 3.0)
    symbol_z = jnp.clip(jax.random.uniform(key_list[4], (GRID_Z,), jnp.float32, 0.3, 3.0), 0.3, 3.0)
    return dict(velocity=velocity, coupling=coupling, symbol_x=symbol_x, symbol_y=symbol_y, symbol_z=symbol_z)


def basis_table(count):
    rank = jnp.arange(count)
    angle = (jnp.pi / (count + 1)) * (((rank[:, None] + 1) * (rank[None, :] + 1)) % (2 * count + 2)).astype(jnp.float32)
    return jnp.sin(angle) * (2.0 / (count + 1)) ** 0.5


def along_dim(values, dim):
    moved = jnp.tensordot(values, basis_table(values.shape[dim]), axes=([dim], [0]), precision=lax.Precision.HIGHEST)
    return jnp.moveaxis(moved, -1, dim)


def reference(velocity, coupling, symbol_x, symbol_y, symbol_z):
    spectrum = velocity
    spectrum = along_dim(spectrum, 1)
    spectrum = along_dim(spectrum, 2)
    spectrum = along_dim(spectrum, 3)
    symbol = symbol_x[:, None, None] + symbol_y[None, :, None] + symbol_z[None, None, :]
    weight_xyz = 1.0 / (1.0 + symbol)
    mixed_fields = jnp.einsum("ab,bxyz->axyz", coupling, spectrum, precision=lax.Precision.HIGHEST)
    spectrum = weight_xyz * spectrum + (1.0 - weight_xyz) * mixed_fields
    return spectrum
```

```python
import functools

import jax
import jax.numpy as jnp
import numpy as np
from jax import lax
from jax.experimental import pallas as pl
from jax.experimental.pallas import tpu as pltpu
from jax.sharding import PartitionSpec as P

LANES = 128
SIZES = (1, 1, 2, 4, 2, 2, 2, 2)
EARLY = 2
HOLD = 4
F32 = jnp.float32
BF16 = jnp.bfloat16
MESH = pl.DeviceIdType.MESH


def basis_table(count):
    rank = np.arange(1, count + 1)
    turns = (rank[:, None] * rank[None, :]) % (2 * count + 2)
    table = np.sin(np.pi / (count + 1) * turns) * (2.0 / (count + 1)) ** 0.5
    table = table.astype(np.float32)
    high = table.astype(jnp.bfloat16)
    low = (table - high.astype(np.float32)).astype(jnp.bfloat16)
    return high, low


def split(values):
    high = values.astype(BF16)
    low = (values - high.astype(F32)).astype(BF16)
    return high, low


def plan(chunks, packs):
    starts = [sum(chunks[:c]) for c in range(len(chunks))]
    early = min(EARLY, len(chunks))
    pieces = [(p, 1, starts[c], chunks[c]) for p in range(packs) for c in range(early)]
    pieces += [(0, packs, starts[c], chunks[c]) for c in range(early, len(chunks))]
    owner = list(range(early)) * packs + list(range(early, len(chunks)))
    return starts, early, pieces, owner


def kernel(
    north, deep, chunks,
    a_hbm, coupling_hbm, sym_x_hbm, sym_y_hbm, sym_z_hbm, tx_hbm, ty_hbm, tz_hbm,
    out,
    a, coupling, sym_x, sym_y, sym_z, tx, ty, tz, x1, r, s, t,
    load_sem, send_n, recv_n, send_d, recv_d, ready,
):
    me_n = lax.axis_index("north")
    me_d = lax.axis_index("deep")
    fields, share_y, share_z, size_x = a.shape
    pack = LANES // share_z
    packs = fields // pack
    share_x = size_x // north
    size_y = share_y * north
    block_y = size_y // deep
    size_z = share_z * deep
    starts, early, pieces, owner = plan(chunks, packs)
    half = deep // 2
    odd = lax.rem(me_n, 2)

    loads = [pltpu.make_async_copy(tx_hbm, tx, load_sem.at[0])]
    for p in range(packs):
        part = pl.ds(p * pack, pack)
        loads.append(pltpu.make_async_copy(a_hbm.at[part], a.at[part], load_sem.at[1 + p]))
    pairs = [
        (ty_hbm, ty), (sym_x_hbm, sym_x), (sym_y_hbm, sym_y), (sym_z_hbm, sym_z),
        (coupling_hbm, coupling), (tz_hbm, tz),
    ]
    late = [
        pltpu.make_async_copy(source, target, load_sem.at[len(loads) + i])
        for i, (source, target) in enumerate(pairs)
    ]
    for copy in loads + late:
        copy.start()

    peers_n = [lax.rem(me_n + k, north) for k in range(1, north)]
    side = me_d // half
    across = [(1 - side) * half + j for j in range(half)]
    along = [side * half + lax.rem(me_d + j, half) for j in range(1, half)]
    peers_d = across + along

    barrier = pltpu.get_barrier_semaphore()
    for k in range(0, north, 2):
        even = lax.rem(me_n - odd + k, north)

        @pl.when(even != me_n)
        def _():
            pl.semaphore_signal(barrier, inc=1, device_id={"north": even}, device_id_type=MESH)

    for peer in peers_d:
        pl.semaphore_signal(
            barrier, inc=1, device_id={"north": me_n - odd + 1, "deep": peer}, device_id_type=MESH
        )

    def enter_north():
        @pl.when(odd == 0)
        def _():
            pl.semaphore_wait(barrier, north - 1)
            pl.semaphore_signal(ready, inc=1, device_id={"north": me_n + 1}, device_id_type=MESH)

        @pl.when(odd == 1)
        def _():
            pl.semaphore_wait(ready, 1)

    def enter_deep():
        @pl.when(odd == 1)
        def _():
            pl.semaphore_wait(barrier, 2 * (deep - 1))
            pl.semaphore_signal(ready, inc=1, device_id={"north": me_n - 1}, device_id_type=MESH)

        @pl.when(odd == 0)
        def _():
            pl.semaphore_wait(ready, 1)

    def north_copy(c, peer):
        p, count, x, size = pieces[c]
        return pltpu.make_async_remote_copy(
            src_ref=x1.at[pl.ds(peer * share_x + x, size), pl.ds(p, count)],
            dst_ref=r.at[me_n, pl.ds(x, size), pl.ds(p, count)],
            send_sem=send_n,
            recv_sem=recv_n.at[c],
            device_id={"north": peer},
            device_id_type=MESH,
        )

    def deep_copy(c, peer):
        p, count, x, size = pieces[c]
        return pltpu.make_async_remote_copy(
            src_ref=s.at[peer, pl.ds(x, size), pl.ds(p, count)],
            dst_ref=t.at[me_d, pl.ds(x, size), pl.ds(p, count)],
            send_sem=send_d,
            recv_sem=recv_d.at[owner[c]],
            device_id={"deep": peer},
            device_id_type=MESH,
        )

    def north_arrived(c):
        p, count, x, size = pieces[c]
        part = r.at[pl.ds(0, north - 1), pl.ds(x, size), pl.ds(p, count)]
        pltpu.make_async_copy(part, part, recv_n.at[c]).wait()

    def deep_arrived(c):
        part = t.at[pl.ds(0, deep - 1), pl.ds(starts[c], chunks[c])]
        pltpu.make_async_copy(part, part, recv_d.at[c]).wait()

    def all_sent():
        part = r.at[pl.ds(0, north - 1)]
        pltpu.make_async_copy(part, part, send_n).wait()
        part = t.at[pl.ds(0, deep - 1)]
        pltpu.make_async_copy(part, part, send_d).wait()

    loads[0].wait()
    for p in range(packs):
        loads[1 + p].wait()
        for y in range(0, share_y, 2):
            rows = [a[p * pack + f, y + i] for i in range(2) for f in range(pack)]
            high, low = split(jnp.concatenate(rows, axis=0))
            lines = lax.dot_general(
                tx[...],
                jnp.concatenate([high, low], axis=1),
                dimension_numbers=(((1,), (1,)), ((), ())),
                preferred_element_type=F32,
            )
            lines = lines[:size_x] + lines[size_x:]
            x1[:, p, y, :] = lines[:, :LANES]
            x1[:, p, y + 1, :] = lines[:, LANES:]
        if p == 0:
            enter_north()
        for c in range(p * early, (p + 1) * early):
            for peer in peers_n:
                north_copy(c, peer).start()

    for c in range(packs * early, len(pieces)):
        for peer in peers_n:
            north_copy(c, peer).start()

    r[me_n] = x1[pl.ds(me_n * share_x, share_x)]

    for copy in late:
        copy.wait()

    rows_y = lax.broadcasted_iota(jnp.int32, (block_y, size_z), 0)
    base = jnp.broadcast_to(sym_z[...], (block_y, size_z))
    column = jnp.zeros((block_y, size_z), F32)
    for i in range(block_y):
        column = jnp.where(rows_y == i, sym_y[0, me_d * block_y + i], column)
    base = base + column

    for c in range(len(pieces)):
        first, count, start, size = pieces[c]
        north_arrived(c)
        for p in range(first, first + count):
            for x in range(start, start + size, 2):
                width = min(2, start + size - x)
                lines = [
                    jnp.concatenate([r[n, x + i, p] for n in range(north)], axis=0)
                    for i in range(width)
                ]
                high, low = split(jnp.concatenate(lines, axis=1))
                stack = jnp.concatenate([high, high, low], axis=0)
                mixed = jnp.dot(ty[...], stack, preferred_element_type=F32)
                for i in range(width):
                    modes = mixed[:, i * LANES:(i + 1) * LANES]
                    for d in range(deep):
                        s[d, x + i, p] = modes[d * block_y:(d + 1) * block_y]
        if c == 0:
            enter_deep()
        now = across[:-1] + along if c == 0 else along + across[:-1]
        for peer in now:
            deep_copy(c, peer).start()
        held = len(pieces) - min(HOLD, len(pieces))
        for k in [c] if c < held else range(held, len(pieces)) if c == len(pieces) - 1 else []:
            deep_copy(k, across[-1]).start()

    t[me_d] = s[me_d]

    for c in range(len(chunks)):
        weights = []
        for x in range(starts[c], starts[c] + chunks[c]):
            weight = 1.0 / (1.0 + (base + sym_x[0, me_n * share_x + x]))
            weights.append((weight, 1.0 - weight))
        deep_arrived(c)
        height = chunks[c] * block_y
        rows = []
        for p in range(packs):
            lines = [
                t[d, starts[c]:starts[c] + chunks[c], p].reshape(height, LANES) for d in range(deep)
            ]
            for f in range(pack):
                rows.append(
                    jnp.concatenate(
                        [line[:, f * share_z:(f + 1) * share_z] for line in lines], axis=1
                    )
                )
        high, low = split(jnp.concatenate(rows, axis=0))
        main = jnp.dot(jnp.concatenate([high, low], axis=0), tz[0], preferred_element_type=F32)
        rest = jnp.dot(high, tz[1], preferred_element_type=F32)
        spectrum = main[:fields * height] + main[fields * height:] + rest
        for i in range(chunks[c]):
            x = starts[c] + i
            weight, other = weights[i]
            old = [
                spectrum[f * height + i * block_y:f * height + (i + 1) * block_y]
                for f in range(fields)
            ]
            for f in range(fields):
                total = coupling[f, 0] * old[0]
                for g in range(1, fields):
                    total = total + coupling[f, g] * old[g]
                out[f, x] = weight * old[f] + other * total

    all_sent()


def on_device(north, deep, velocity, coupling, symbol_x, symbol_y, symbol_z):
    field = jnp.transpose(velocity, (0, 2, 3, 1))
    fields, share_y, share_z, size_x = field.shape
    size_y, size_z = share_y * north, share_z * deep
    share_x, block_y = size_x // north, size_y // deep
    packs = fields * share_z // LANES
    unit = sum(SIZES)
    chunks = [size * share_x // unit for size in SIZES] if share_x % unit == 0 else [share_x]
    count = len(plan(chunks, packs)[2])
    high, low = basis_table(size_x)
    tx = jnp.asarray(np.block([[high, high], [low, np.zeros_like(low)]]))
    high, low = basis_table(size_y)
    ty = jnp.asarray(np.concatenate([high, low, high], axis=1))
    high, low = basis_table(size_z)
    tz = jnp.asarray(np.stack([high, low]))
    need = 4 * field.size * 7 + 2 * (tx.size + ty.size + tz.size) + 2**21
    vmem = pl.BlockSpec(memory_space=pltpu.VMEM)
    hbm = pl.BlockSpec(memory_space=pltpu.HBM)
    operands = (field, coupling, symbol_x[None, :], symbol_y[None, :], symbol_z[None, :], tx, ty, tz)
    return pl.pallas_call(
        functools.partial(kernel, north, deep, chunks),
        out_shape=jax.ShapeDtypeStruct((fields, share_x, block_y, size_z), F32),
        in_specs=[hbm] * 8,
        out_specs=vmem,
        scratch_shapes=[
            pltpu.VMEM(field.shape, F32),
            pltpu.SMEM(coupling.shape, F32),
            pltpu.SMEM((1, size_x), F32),
            pltpu.SMEM((1, size_y), F32),
            pltpu.VMEM((1, size_z), F32),
            pltpu.VMEM(tx.shape, BF16),
            pltpu.VMEM(ty.shape, BF16),
            pltpu.VMEM(tz.shape, BF16),
            pltpu.VMEM((size_x, packs, share_y, LANES), F32),
            pltpu.VMEM((north, share_x, packs, share_y, LANES), F32),
            pltpu.VMEM((deep, share_x, packs, block_y, LANES), F32),
            pltpu.VMEM((deep, share_x, packs, block_y, LANES), F32),
            pltpu.SemaphoreType.DMA((7 + packs,)),
            pltpu.SemaphoreType.DMA,
            pltpu.SemaphoreType.DMA((count,)),
            pltpu.SemaphoreType.DMA,
            pltpu.SemaphoreType.DMA((len(chunks),)),
            pltpu.SemaphoreType.REGULAR,
        ],
        compiler_params=pltpu.CompilerParams(
            collective_id=0, has_side_effects=True, vmem_limit_bytes=need
        ),
    )(*[pltpu.with_memory_space_constraint(v, pltpu.HBM) for v in operands])


def solution(mesh):
    placed = (P(None, None, "north", "deep"), P(), P(), P(), P())
    return jax.shard_map(
        functools.partial(on_device, mesh.shape["north"], mesh.shape["deep"]),
        mesh=mesh,
        in_specs=placed,
        out_specs=P(None, "north", "deep", None),
        check_vma=False,
    )
```

```python
import functools

import jax
import jax.numpy as jnp
import numpy as np
from jax import lax
from jax.experimental import pallas as pl
from jax.experimental.pallas import tpu as pltpu
from jax.sharding import PartitionSpec as P

LANES = 128
SIZES = (1, 1, 2, 2, 3, 2, 2, 2, 1)
EARLY = 2
HOLD = 4
PASS = 5
LENT = 4
F32 = jnp.float32
BF16 = jnp.bfloat16
MESH = pl.DeviceIdType.MESH


def basis_table(count):
    rank = np.arange(1, count + 1)
    turns = (rank[:, None] * rank[None, :]) % (2 * count + 2)
    table = np.sin(np.pi / (count + 1) * turns) * (2.0 / (count + 1)) ** 0.5
    table = table.astype(np.float32)
    high = table.astype(jnp.bfloat16)
    low = (table - high.astype(np.float32)).astype(jnp.bfloat16)
    return high, low


def split(values):
    high = values.astype(BF16)
    low = (values - high.astype(F32)).astype(BF16)
    return high, low


def plan(chunks, packs):
    starts = [sum(chunks[:c]) for c in range(len(chunks))]
    early = min(EARLY, len(chunks))
    pieces = [(p, 1, starts[c], chunks[c]) for p in range(packs) for c in range(early)]
    pieces += [(0, packs, starts[c], chunks[c]) for c in range(early, len(chunks))]
    owner = list(range(early)) * packs + list(range(early, len(chunks)))
    return starts, early, pieces, owner


def kernel(
    north, deep, chunks,
    a_hbm, coupling_hbm, sym_x_hbm, sym_y_hbm, sym_z_hbm, tx_hbm, ty_hbm, tz_hbm,
    out,
    a, coupling, sym_x, sym_y, sym_z, tx, ty, tz, x1, r, s, t,
    given, r_given, s_given,
    load_sem, send_n, recv_n, send_d, recv_d, ready,
    send_lent, send_give, recv_give, send_pass, recv_pass, send_given,
):
    me_n = lax.axis_index("north")
    me_d = lax.axis_index("deep")
    fields, share_y, share_z, size_x = a.shape
    pack = LANES // share_z
    packs = fields // pack
    share_x = size_x // north
    size_y = share_y * north
    block_y = size_y // deep
    size_z = share_z * deep
    starts, early, pieces, owner = plan(chunks, packs)
    half = deep // 2
    last = len(pieces) - 1
    split_x = len(chunks) > LENT
    lent = owner.index(LENT) if split_x else -1
    first_x, shared = (starts[LENT], chunks[LENT]) if split_x else (0, 1)
    giver, taker = half, half - 1
    odd = lax.rem(me_n, 2)

    loads = [pltpu.make_async_copy(tx_hbm, tx, load_sem.at[0])]
    for p in range(packs):
        part = pl.ds(p * pack, pack)
        loads.append(pltpu.make_async_copy(a_hbm.at[part], a.at[part], load_sem.at[1 + p]))
    pairs = [
        (ty_hbm, ty), (sym_x_hbm, sym_x), (sym_y_hbm, sym_y), (sym_z_hbm, sym_z),
        (coupling_hbm, coupling), (tz_hbm, tz),
    ]
    late = [
        pltpu.make_async_copy(source, target, load_sem.at[len(loads) + i])
        for i, (source, target) in enumerate(pairs)
    ]
    for copy in loads + late:
        copy.start()

    peers_n = [lax.rem(me_n + k, north) for k in range(1, north)]
    side = me_d // half
    across = [(1 - side) * half + j for j in range(half)]
    along = [side * half + lax.rem(me_d + j, half) for j in range(1, half)]
    peers_d = across + along

    barrier = pltpu.get_barrier_semaphore()
    for k in range(0, north, 2):
        even = lax.rem(me_n - odd + k, north)

        @pl.when(even != me_n)
        def _():
            pl.semaphore_signal(barrier, inc=1, device_id={"north": even}, device_id_type=MESH)

    @pl.when(odd == 0)
    def _():
        pl.semaphore_signal(barrier, inc=1, device_id={"north": me_n + 1}, device_id_type=MESH)

    for peer in peers_d:
        pl.semaphore_signal(
            barrier, inc=1, device_id={"north": me_n - odd + 1, "deep": peer}, device_id_type=MESH
        )

    def gather_north():
        pl.semaphore_wait(barrier, north - 1)
        pl.semaphore_signal(ready, inc=1, device_id={"north": me_n + 1}, device_id_type=MESH)

    def gather_deep():
        pl.semaphore_wait(barrier, 2 * (deep - 1) + 1)
        pl.semaphore_signal(ready, inc=1, device_id={"north": me_n - 1}, device_id_type=MESH)

    def be_ready():
        pl.semaphore_wait(ready, 1)

    gives = lax.convert_element_type(me_d == giver, jnp.int32) if split_x else 0

    def enter_north():
        pl.when(odd == 0)(gather_north)
        pl.when(odd * gives == 1)(gather_deep)
        pl.when(odd == 1)(be_ready)

    def enter_deep():
        pl.when(odd * (1 - gives) == 1)(gather_deep)
        pl.when(odd == 0)(be_ready)

    def north_copy(c, peer):
        p, count, x, size = pieces[c]
        return pltpu.make_async_remote_copy(
            src_ref=x1.at[pl.ds(peer * share_x + x, size), pl.ds(p, count)],
            dst_ref=r.at[me_n, pl.ds(x, size), pl.ds(p, count)],
            send_sem=send_n,
            recv_sem=recv_n.at[c],
            device_id={"north": peer},
            device_id_type=MESH,
        )

    def deep_copy(c, peer):
        p, count, x, size = pieces[c]
        return pltpu.make_async_remote_copy(
            src_ref=s.at[peer, pl.ds(x, size), pl.ds(p, count)],
            dst_ref=t.at[me_d, pl.ds(x, size), pl.ds(p, count)],
            send_sem=send_lent if c == lent else send_d,
            recv_sem=recv_d.at[owner[c]],
            device_id={"deep": peer},
            device_id_type=MESH,
        )

    def give(p, k):
        return pltpu.make_async_remote_copy(
            src_ref=x1.at[pl.ds(k * share_x + first_x, shared), pl.ds(p, 1)],
            dst_ref=given.at[k, pl.ds(0, shared), pl.ds(p, 1)],
            send_sem=send_give,
            recv_sem=recv_give,
            device_id={"deep": taker},
            device_id_type=MESH,
        )

    def pass_on(peer):
        return pltpu.make_async_remote_copy(
            src_ref=given.at[peer],
            dst_ref=r_given.at[me_n],
            send_sem=send_pass,
            recv_sem=recv_pass,
            device_id={"north": peer},
            device_id_type=MESH,
        )

    def hand_over(peer):
        return pltpu.make_async_remote_copy(
            src_ref=s_given.at[peer],
            dst_ref=t.at[giver, pl.ds(first_x, shared)],
            send_sem=send_given,
            recv_sem=recv_d.at[LENT],
            device_id={"deep": peer},
            device_id_type=MESH,
        )

    def take(ref, sem):
        pltpu.make_async_copy(ref, ref, sem).wait()

    def north_arrived(c):
        p, count, x, size = pieces[c]
        take(r.at[pl.ds(0, north - 1), pl.ds(x, size), pl.ds(p, count)], recv_n.at[c])

    def deep_arrived(c):
        take(t.at[pl.ds(0, deep - 1), pl.ds(starts[c], chunks[c])], recv_d.at[c])

    def all_sent():
        take(r.at[pl.ds(0, north - 1)], send_n)
        if not split_x:
            take(t.at[pl.ds(0, deep - 1)], send_d)
            return
        take(t.at[pl.ds(0, deep - 1), pl.ds(0, share_x - shared)], send_d)

        @pl.when(me_d == giver)
        def _():
            if half > 1:
                take(t.at[pl.ds(0, half - 1), pl.ds(first_x, shared)], send_lent)
            take(given, send_give)

        @pl.when(me_d != giver)
        def _():
            take(t.at[pl.ds(0, deep - 1), pl.ds(first_x, shared)], send_lent)

        @pl.when(me_d == taker)
        def _():
            take(given.at[pl.ds(0, north - 1)], send_pass)
            if half > 1:
                take(s_given.at[pl.ds(0, half - 1)], send_given)

    def to_modes(source, target, first, count, start, stop):
        for p in range(first, first + count):
            for x in range(start, stop, 2):
                width = min(2, stop - x)
                lines = [
                    jnp.concatenate([source[n, x + i, p] for n in range(north)], axis=0)
                    for i in range(width)
                ]
                high, low = split(jnp.concatenate(lines, axis=1))
                stack = jnp.concatenate([high, high, low], axis=0)
                mixed = jnp.dot(ty[...], stack, preferred_element_type=F32)
                for i in range(width):
                    modes = mixed[:, i * LANES:(i + 1) * LANES]
                    for d in range(deep):
                        target[d, x + i, p] = modes[d * block_y:(d + 1) * block_y]

    loads[0].wait()
    for p in range(packs):
        loads[1 + p].wait()
        for y in range(0, share_y, 2):
            rows = [a[p * pack + f, y + i] for i in range(2) for f in range(pack)]
            high, low = split(jnp.concatenate(rows, axis=0))
            lines = lax.dot_general(
                tx[...],
                jnp.concatenate([high, low], axis=1),
                dimension_numbers=(((1,), (1,)), ((), ())),
                preferred_element_type=F32,
            )
            lines = lines[:size_x] + lines[size_x:]
            x1[:, p, y, :] = lines[:, :LANES]
            x1[:, p, y + 1, :] = lines[:, LANES:]
        if p == 0:
            enter_north()
        sent = range(p * early, (p + 1) * early if p < packs - 1 else len(pieces))
        for c in sent:
            for peer in peers_n:
                north_copy(c, peer).start()
        if split_x:
            @pl.when(me_d == giver)
            def _():
                if p == 0:
                    enter_deep()
                for k in range(north):
                    give(p, k).start()

    r[me_n] = x1[pl.ds(me_n * share_x, share_x)]

    for copy in late:
        copy.wait()

    rows_y = lax.broadcasted_iota(jnp.int32, (block_y, size_z), 0)
    base = jnp.broadcast_to(sym_z[...], (block_y, size_z))
    column = jnp.zeros((block_y, size_z), F32)
    for i in range(block_y):
        column = jnp.where(rows_y == i, sym_y[0, me_d * block_y + i], column)
    base = base + column

    for c in range(len(pieces)):
        first, count, start, size = pieces[c]
        if c == 0:
            if split_x:
                pl.when(me_d != giver)(enter_deep)
            else:
                enter_deep()
        north_arrived(c)
        to_modes(r, s, first, count, start, start + size)
        crossing = [(c, peer, True) for peer in across[:-1]]
        beside = [(c, peer, False) for peer in along]
        now = crossing + beside if c == 0 else beside + crossing
        held = len(pieces) - min(HOLD, len(pieces))
        then = [c] if c < held else range(held, len(pieces)) if c == last else []
        for k, peer, crosses in now + [(k, across[-1], True) for k in then]:
            copy = deep_copy(k, peer)
            if k == lent and crosses:
                pl.when(me_d != giver)(copy.start)
            else:
                copy.start()

        if split_x and c == min(PASS, last):
            @pl.when(me_d == taker)
            def _():
                take(given, recv_give)
                for peer in peers_n:
                    pass_on(peer).start()
                r_given[me_n] = given[me_n]

    if split_x:
        @pl.when(me_d == taker)
        def _():
            take(r_given.at[pl.ds(0, north - 1)], recv_pass)
            to_modes(r_given, s_given, 0, packs, 0, shared)
            for peer in along:
                hand_over(peer).start()
            pltpu.make_async_copy(
                s_given.at[me_d], t.at[giver, pl.ds(first_x, shared)], recv_d.at[LENT]
            ).start()

    t[me_d] = s[me_d]

    for c in range(len(chunks)):
        weights = []
        for x in range(starts[c], starts[c] + chunks[c]):
            weight = 1.0 / (1.0 + (base + sym_x[0, me_n * share_x + x]))
            weights.append((weight, 1.0 - weight))
        deep_arrived(c)
        height = chunks[c] * block_y
        rows = []
        for p in range(packs):
            lines = [
                t[d, starts[c]:starts[c] + chunks[c], p].reshape(height, LANES) for d in range(deep)
            ]
            for f in range(pack):
                rows.append(
                    jnp.concatenate(
                        [line[:, f * share_z:(f + 1) * share_z] for line in lines], axis=1
                    )
                )
        high, low = split(jnp.concatenate(rows, axis=0))
        main = jnp.dot(jnp.concatenate([high, low], axis=0), tz[0], preferred_element_type=F32)
        rest = jnp.dot(high, tz[1], preferred_element_type=F32)
        spectrum = main[:fields * height] + main[fields * height:] + rest
        for i in range(chunks[c]):
            x = starts[c] + i
            weight, other = weights[i]
            old = [
                spectrum[f * height + i * block_y:f * height + (i + 1) * block_y]
                for f in range(fields)
            ]
            for f in range(fields):
                total = coupling[f, 0] * old[0]
                for g in range(1, fields):
                    total = total + coupling[f, g] * old[g]
                out[f, x] = weight * old[f] + other * total

    all_sent()


def on_device(north, deep, velocity, coupling, symbol_x, symbol_y, symbol_z):
    field = jnp.transpose(velocity, (0, 2, 3, 1))
    fields, share_y, share_z, size_x = field.shape
    size_y, size_z = share_y * north, share_z * deep
    share_x, block_y = size_x // north, size_y // deep
    packs = fields * share_z // LANES
    unit = sum(SIZES)
    chunks = [size * share_x // unit for size in SIZES] if share_x % unit == 0 else [share_x]
    count = len(plan(chunks, packs)[2])
    lent = chunks[LENT] if len(chunks) > LENT else 1
    high, low = basis_table(size_x)
    tx = jnp.asarray(np.block([[high, high], [low, np.zeros_like(low)]]))
    high, low = basis_table(size_y)
    ty = jnp.asarray(np.concatenate([high, low, high], axis=1))
    high, low = basis_table(size_z)
    tz = jnp.asarray(np.stack([high, low]))
    need = 4 * field.size * 8 + 2 * (tx.size + ty.size + tz.size) + 2**21
    vmem = pl.BlockSpec(memory_space=pltpu.VMEM)
    hbm = pl.BlockSpec(memory_space=pltpu.HBM)
    operands = (field, coupling, symbol_x[None, :], symbol_y[None, :], symbol_z[None, :], tx, ty, tz)
    return pl.pallas_call(
        functools.partial(kernel, north, deep, chunks),
        out_shape=jax.ShapeDtypeStruct((fields, share_x, block_y, size_z), F32),
        in_specs=[hbm] * 8,
        out_specs=vmem,
        scratch_shapes=[
            pltpu.VMEM(field.shape, F32),
            pltpu.SMEM(coupling.shape, F32),
            pltpu.SMEM((1, size_x), F32),
            pltpu.SMEM((1, size_y), F32),
            pltpu.VMEM((1, size_z), F32),
            pltpu.VMEM(tx.shape, BF16),
            pltpu.VMEM(ty.shape, BF16),
            pltpu.VMEM(tz.shape, BF16),
            pltpu.VMEM((size_x, packs, share_y, LANES), F32),
            pltpu.VMEM((north, share_x, packs, share_y, LANES), F32),
            pltpu.VMEM((deep, share_x, packs, block_y, LANES), F32),
            pltpu.VMEM((deep, share_x, packs, block_y, LANES), F32),
            pltpu.VMEM((north, lent, packs, share_y, LANES), F32),
            pltpu.VMEM((north, lent, packs, share_y, LANES), F32),
            pltpu.VMEM((deep, lent, packs, block_y, LANES), F32),
            pltpu.SemaphoreType.DMA((7 + packs,)),
            pltpu.SemaphoreType.DMA,
            pltpu.SemaphoreType.DMA((count,)),
            pltpu.SemaphoreType.DMA,
            pltpu.SemaphoreType.DMA((len(chunks),)),
            pltpu.SemaphoreType.REGULAR,
            pltpu.SemaphoreType.DMA,
            pltpu.SemaphoreType.DMA,
            pltpu.SemaphoreType.DMA,
            pltpu.SemaphoreType.DMA,
            pltpu.SemaphoreType.DMA,
            pltpu.SemaphoreType.DMA,
        ],
        compiler_params=pltpu.CompilerParams(
            collective_id=0, has_side_effects=True, vmem_limit_bytes=need
        ),
    )(*[pltpu.with_memory_space_constraint(v, pltpu.HBM) for v in operands])


def solution(mesh):
    placed = (P(None, None, "north", "deep"), P(), P(), P(), P())
    return jax.shard_map(
        functools.partial(on_device, mesh.shape["north"], mesh.shape["deep"]),
        mesh=mesh,
        in_specs=placed,
        out_specs=P(None, "north", "deep", None),
        check_vma=False,
    )
```

```python
import functools

import jax
import jax.numpy as jnp
import numpy as np
from jax import lax
from jax.experimental import pallas as pl
from jax.experimental.pallas import tpu as pltpu
from jax.sharding import PartitionSpec as P

LANES = 128
SIZES = (1, 1, 2, 2, 3, 2, 2, 2, 1)
EARLY = 2
HOLD = 5
PASS = 4
LENT = 4
F32 = jnp.float32
BF16 = jnp.bfloat16
MESH = pl.DeviceIdType.MESH


def basis_table(count):
    rank = np.arange(1, count + 1)
    turns = (rank[:, None] * rank[None, :]) % (2 * count + 2)
    table = np.sin(np.pi / (count + 1) * turns) * (2.0 / (count + 1)) ** 0.5
    table = table.astype(np.float32)
    high = table.astype(jnp.bfloat16)
    low = (table - high.astype(np.float32)).astype(jnp.bfloat16)
    return high, low


def split(values):
    high = values.astype(BF16)
    low = (values - high.astype(F32)).astype(BF16)
    return high, low


def plan(chunks, packs):
    starts = [sum(chunks[:c]) for c in range(len(chunks))]
    early = min(EARLY, len(chunks))
    pieces = [(p, 1, starts[c], chunks[c]) for p in range(packs) for c in range(early)]
    pieces += [(0, packs, starts[c], chunks[c]) for c in range(early, len(chunks))]
    owner = list(range(early)) * packs + list(range(early, len(chunks)))
    return starts, early, pieces, owner


def kernel(
    north, deep, chunks,
    a_hbm, coupling_hbm, sym_x_hbm, sym_y_hbm, sym_z_hbm, tx_hbm, ty_hbm, tz_hbm,
    out,
    a, coupling, sym_x, sym_y, sym_z, tx, ty, tz, x1, r, s, t,
    given, r_given, s_given,
    load_sem, send_n, recv_n, send_d, recv_d, ready,
    send_lent, send_give, recv_give, send_pass, recv_pass, send_given,
):
    me_n = lax.axis_index("north")
    me_d = lax.axis_index("deep")
    fields, share_y, share_z, size_x = a.shape
    pack = LANES // share_z
    packs = fields // pack
    share_x = size_x // north
    size_y = share_y * north
    block_y = size_y // deep
    size_z = share_z * deep
    starts, early, pieces, owner = plan(chunks, packs)
    half = deep // 2
    last = len(pieces) - 1
    split_x = len(chunks) > LENT
    lent = owner.index(LENT) if split_x else -1
    first_x, shared = (starts[LENT], chunks[LENT]) if split_x else (0, 1)
    upper, lower = me_d == half, me_d == half - 1
    inner, partner = upper | lower, deep - 1 - me_d
    odd = lax.rem(me_n, 2)

    loads = [pltpu.make_async_copy(tx_hbm, tx, load_sem.at[0])]
    for p in range(packs):
        part = pl.ds(p * pack, pack)
        loads.append(pltpu.make_async_copy(a_hbm.at[part], a.at[part], load_sem.at[1 + p]))
    pairs = [
        (ty_hbm, ty), (sym_x_hbm, sym_x), (sym_y_hbm, sym_y), (sym_z_hbm, sym_z),
        (coupling_hbm, coupling), (tz_hbm, tz),
    ]
    late = [
        pltpu.make_async_copy(source, target, load_sem.at[len(loads) + i])
        for i, (source, target) in enumerate(pairs)
    ]
    for copy in loads + late:
        copy.start()

    peers_n = [lax.rem(me_n + k, north) for k in range(1, north)]
    side = me_d // half
    across = [(1 - side) * (deep - 1 - j) + side * j for j in range(half)]
    along = [side * half + lax.rem(me_d + j, half) for j in range(1, half)]
    peers_d = across + along

    barrier = pltpu.get_barrier_semaphore()
    for k in range(0, north, 2):
        even = lax.rem(me_n - odd + k, north)

        @pl.when(even != me_n)
        def _():
            pl.semaphore_signal(barrier, inc=1, device_id={"north": even}, device_id_type=MESH)

    @pl.when(odd == 0)
    def _():
        pl.semaphore_signal(barrier, inc=1, device_id={"north": me_n + 1}, device_id_type=MESH)

    for peer in peers_d:
        pl.semaphore_signal(
            barrier, inc=1, device_id={"north": me_n - odd + 1, "deep": peer}, device_id_type=MESH
        )

    def gather_north():
        pl.semaphore_wait(barrier, north - 1)
        pl.semaphore_signal(ready, inc=1, device_id={"north": me_n + 1}, device_id_type=MESH)

    def gather_deep():
        pl.semaphore_wait(barrier, 2 * (deep - 1) + 1)
        pl.semaphore_signal(ready, inc=1, device_id={"north": me_n - 1}, device_id_type=MESH)

    def be_ready():
        pl.semaphore_wait(ready, 1)

    def enter_north():
        pl.when(odd == 0)(gather_north)
        pl.when(odd == 1)(be_ready)

    def enter_deep():
        pl.when(odd == 1)(gather_deep)
        pl.when(odd == 0)(be_ready)

    def north_copy(c, peer):
        p, count, x, size = pieces[c]
        return pltpu.make_async_remote_copy(
            src_ref=x1.at[pl.ds(peer * share_x + x, size), pl.ds(p, count)],
            dst_ref=r.at[me_n, pl.ds(x, size), pl.ds(p, count)],
            send_sem=send_n,
            recv_sem=recv_n.at[c],
            device_id={"north": peer},
            device_id_type=MESH,
        )

    def deep_copy(c, peer):
        p, count, x, size = pieces[c]
        return pltpu.make_async_remote_copy(
            src_ref=s.at[peer, pl.ds(x, size), pl.ds(p, count)],
            dst_ref=t.at[me_d, pl.ds(x, size), pl.ds(p, count)],
            send_sem=send_lent if c == lent else send_d,
            recv_sem=recv_d.at[owner[c]],
            device_id={"deep": peer},
            device_id_type=MESH,
        )

    def give(given_packs):
        for p in given_packs:
            for k in range(north):
                pltpu.make_async_remote_copy(
                    src_ref=x1.at[pl.ds(k * share_x + first_x, shared), pl.ds(p, 1)],
                    dst_ref=given.at[k, pl.ds(0, shared), pl.ds(p, 1)],
                    send_sem=send_give,
                    recv_sem=recv_give,
                    device_id={"deep": partner},
                    device_id_type=MESH,
                ).start()

    def enter_and_give(given_packs):
        enter_deep()
        give(given_packs)

    def pass_on(peer):
        return pltpu.make_async_remote_copy(
            src_ref=given.at[peer],
            dst_ref=r_given.at[me_n],
            send_sem=send_pass,
            recv_sem=recv_pass,
            device_id={"north": peer},
            device_id_type=MESH,
        )

    def hand_over(peer):
        return pltpu.make_async_remote_copy(
            src_ref=s_given.at[peer],
            dst_ref=t.at[partner, pl.ds(first_x, shared)],
            send_sem=send_given,
            recv_sem=recv_d.at[LENT],
            device_id={"deep": peer},
            device_id_type=MESH,
        )

    def take_and_pass():
        take(given, recv_give)
        for peer in peers_n:
            pass_on(peer).start()
        r_given[me_n] = given[me_n]

    def take(ref, sem):
        pltpu.make_async_copy(ref, ref, sem).wait()

    def north_arrived(c):
        p, count, x, size = pieces[c]
        take(r.at[pl.ds(0, north - 1), pl.ds(x, size), pl.ds(p, count)], recv_n.at[c])

    def deep_arrived(c):
        take(t.at[pl.ds(0, deep - 1), pl.ds(starts[c], chunks[c])], recv_d.at[c])

    def all_sent():
        take(r.at[pl.ds(0, north - 1)], send_n)
        if not split_x:
            take(t.at[pl.ds(0, deep - 1)], send_d)
            return
        take(t.at[pl.ds(0, deep - 1), pl.ds(0, share_x - shared)], send_d)

        @pl.when(inner)
        def _():
            take(given, send_give)
            take(given.at[pl.ds(0, north - 1)], send_pass)
            if half > 1:
                take(t.at[pl.ds(0, half - 1), pl.ds(first_x, shared)], send_lent)
                take(s_given.at[pl.ds(0, half - 1)], send_given)

        @pl.when(jnp.logical_not(inner))
        def _():
            take(t.at[pl.ds(0, deep - 1), pl.ds(first_x, shared)], send_lent)

    def to_modes(source, target, first, count, start, stop):
        for p in range(first, first + count):
            for x in range(start, stop, 2):
                width = min(2, stop - x)
                lines = [
                    jnp.concatenate([source[n, x + i, p] for n in range(north)], axis=0)
                    for i in range(width)
                ]
                high, low = split(jnp.concatenate(lines, axis=1))
                stack = jnp.concatenate([high, high, low], axis=0)
                mixed = jnp.dot(ty[...], stack, preferred_element_type=F32)
                for i in range(width):
                    modes = mixed[:, i * LANES:(i + 1) * LANES]
                    for d in range(deep):
                        target[d, x + i, p] = modes[d * block_y:(d + 1) * block_y]

    loads[0].wait()
    for p in range(packs):
        loads[1 + p].wait()
        for y in range(0, share_y, 2):
            rows = [a[p * pack + f, y + i] for i in range(2) for f in range(pack)]
            high, low = split(jnp.concatenate(rows, axis=0))
            lines = lax.dot_general(
                tx[...],
                jnp.concatenate([high, low], axis=1),
                dimension_numbers=(((1,), (1,)), ((), ())),
                preferred_element_type=F32,
            )
            lines = lines[:size_x] + lines[size_x:]
            x1[:, p, y, :] = lines[:, :LANES]
            x1[:, p, y + 1, :] = lines[:, LANES:]
        if p == 0:
            waits = me_n < north - 2
            if split_x:
                pl.when(upper & waits)(functools.partial(enter_and_give, [p]))
            enter_north()
        sent = range(p * early, (p + 1) * early if p < packs - 1 else len(pieces))
        for c in sent:
            for peer in peers_n:
                north_copy(c, peer).start()
        if split_x and p == 0:
            pl.when(upper & jnp.logical_not(waits))(functools.partial(enter_and_give, [p]))
        elif split_x:
            pl.when(upper)(functools.partial(give, [p]))
    if split_x:
        pl.when(lower)(functools.partial(enter_and_give, range(packs)))

    r[me_n] = x1[pl.ds(me_n * share_x, share_x)]

    for copy in late:
        copy.wait()

    rows_y = lax.broadcasted_iota(jnp.int32, (block_y, size_z), 0)
    base = jnp.broadcast_to(sym_z[...], (block_y, size_z))
    column = jnp.zeros((block_y, size_z), F32)
    for i in range(block_y):
        column = jnp.where(rows_y == i, sym_y[0, me_d * block_y + i], column)
    base = base + column

    for c in range(len(pieces)):
        first, count, start, size = pieces[c]
        if c == 0:
            if split_x:
                pl.when(jnp.logical_not(inner))(enter_deep)
            else:
                enter_deep()
        north_arrived(c)
        to_modes(r, s, first, count, start, start + size)
        crossing = [(c, peer, True) for peer in across[:-1]]
        beside = [(c, peer, False) for peer in along]
        now = crossing + beside if c == 0 else beside + crossing
        held = len(pieces) - min(HOLD, len(pieces))
        then = [c] if c < held else range(held, len(pieces)) if c == last else []
        for k, peer, crosses in now + [(k, across[-1], True) for k in then]:
            copy = deep_copy(k, peer)
            if k == lent and crosses:
                pl.when(jnp.logical_not(inner))(copy.start)
            else:
                copy.start()

        if split_x and c == min(PASS, last):
            pl.when(lower)(take_and_pass)

    if split_x:
        pl.when(upper)(take_and_pass)

    if split_x:
        @pl.when(inner)
        def _():
            take(r_given.at[pl.ds(0, north - 1)], recv_pass)
            to_modes(r_given, s_given, 0, packs, 0, shared)
            for peer in along:
                hand_over(peer).start()
            pltpu.make_async_copy(
                s_given.at[me_d], t.at[partner, pl.ds(first_x, shared)], recv_d.at[LENT]
            ).start()

    t[me_d] = s[me_d]

    for c in range(len(chunks)):
        weights = []
        for x in range(starts[c], starts[c] + chunks[c]):
            weight = 1.0 / (1.0 + (base + sym_x[0, me_n * share_x + x]))
            weights.append((weight, 1.0 - weight))
        deep_arrived(c)
        height = chunks[c] * block_y
        rows = []
        for p in range(packs):
            lines = [
                t[d, starts[c]:starts[c] + chunks[c], p].reshape(height, LANES) for d in range(deep)
            ]
            for f in range(pack):
                rows.append(
                    jnp.concatenate(
                        [line[:, f * share_z:(f + 1) * share_z] for line in lines], axis=1
                    )
                )
        high, low = split(jnp.concatenate(rows, axis=0))
        main = jnp.dot(jnp.concatenate([high, low], axis=0), tz[0], preferred_element_type=F32)
        rest = jnp.dot(high, tz[1], preferred_element_type=F32)
        spectrum = main[:fields * height] + main[fields * height:] + rest
        for i in range(chunks[c]):
            x = starts[c] + i
            weight, other = weights[i]
            old = [
                spectrum[f * height + i * block_y:f * height + (i + 1) * block_y]
                for f in range(fields)
            ]
            for f in range(fields):
                total = coupling[f, 0] * old[0]
                for g in range(1, fields):
                    total = total + coupling[f, g] * old[g]
                out[f, x] = weight * old[f] + other * total

    all_sent()


def on_device(north, deep, velocity, coupling, symbol_x, symbol_y, symbol_z):
    field = jnp.transpose(velocity, (0, 2, 3, 1))
    fields, share_y, share_z, size_x = field.shape
    size_y, size_z = share_y * north, share_z * deep
    share_x, block_y = size_x // north, size_y // deep
    packs = fields * share_z // LANES
    unit = sum(SIZES)
    chunks = [size * share_x // unit for size in SIZES] if share_x % unit == 0 else [share_x]
    count = len(plan(chunks, packs)[2])
    lent = chunks[LENT] if len(chunks) > LENT else 1
    high, low = basis_table(size_x)
    tx = jnp.asarray(np.block([[high, high], [low, np.zeros_like(low)]]))
    high, low = basis_table(size_y)
    ty = jnp.asarray(np.concatenate([high, low, high], axis=1))
    high, low = basis_table(size_z)
    tz = jnp.asarray(np.stack([high, low]))
    need = 4 * field.size * 8 + 2 * (tx.size + ty.size + tz.size) + 2**21
    vmem = pl.BlockSpec(memory_space=pltpu.VMEM)
    hbm = pl.BlockSpec(memory_space=pltpu.HBM)
    operands = (field, coupling, symbol_x[None, :], symbol_y[None, :], symbol_z[None, :], tx, ty, tz)
    return pl.pallas_call(
        functools.partial(kernel, north, deep, chunks),
        out_shape=jax.ShapeDtypeStruct((fields, share_x, block_y, size_z), F32),
        in_specs=[hbm] * 8,
        out_specs=vmem,
        scratch_shapes=[
            pltpu.VMEM(field.shape, F32),
            pltpu.SMEM(coupling.shape, F32),
            pltpu.SMEM((1, size_x), F32),
            pltpu.SMEM((1, size_y), F32),
            pltpu.VMEM((1, size_z), F32),
            pltpu.VMEM(tx.shape, BF16),
            pltpu.VMEM(ty.shape, BF16),
            pltpu.VMEM(tz.shape, BF16),
            pltpu.VMEM((size_x, packs, share_y, LANES), F32),
            pltpu.VMEM((north, share_x, packs, share_y, LANES), F32),
            pltpu.VMEM((deep, share_x, packs, block_y, LANES), F32),
            pltpu.VMEM((deep, share_x, packs, block_y, LANES), F32),
            pltpu.VMEM((north, lent, packs, share_y, LANES), F32),
            pltpu.VMEM((north, lent, packs, share_y, LANES), F32),
            pltpu.VMEM((deep, lent, packs, block_y, LANES), F32),
            pltpu.SemaphoreType.DMA((7 + packs,)),
            pltpu.SemaphoreType.DMA,
            pltpu.SemaphoreType.DMA((count,)),
            pltpu.SemaphoreType.DMA,
            pltpu.SemaphoreType.DMA((len(chunks),)),
            pltpu.SemaphoreType.REGULAR,
            pltpu.SemaphoreType.DMA,
            pltpu.SemaphoreType.DMA,
            pltpu.SemaphoreType.DMA,
            pltpu.SemaphoreType.DMA,
            pltpu.SemaphoreType.DMA,
            pltpu.SemaphoreType.DMA,
        ],
        compiler_params=pltpu.CompilerParams(
            collective_id=0, has_side_effects=True, vmem_limit_bytes=need
        ),
    )(*[pltpu.with_memory_space_constraint(v, pltpu.HBM) for v in operands])


def solution(mesh):
    placed = (P(None, None, "north", "deep"), P(), P(), P(), P())
    return jax.shard_map(
        functools.partial(on_device, mesh.shape["north"], mesh.shape["deep"]),
        mesh=mesh,
        in_specs=placed,
        out_specs=P(None, "north", "deep", None),
        check_vma=False,
    )
```

```python
import functools

import jax
import jax.numpy as jnp
import numpy as np
from jax import lax
from jax.experimental import pallas as pl
from jax.experimental.pallas import tpu as pltpu
from jax.sharding import PartitionSpec as P

LANES = 128
SIZES = (1, 1, 2, 2, 2, 1, 2, 2, 2, 1)
EARLY = 2
HOLD = 5
PASS = 6
LENT = 4
F32 = jnp.float32
BF16 = jnp.bfloat16
MESH = pl.DeviceIdType.MESH


def basis_table(count):
    rank = np.arange(1, count + 1)
    turns = (rank[:, None] * rank[None, :]) % (2 * count + 2)
    table = np.sin(np.pi / (count + 1) * turns) * (2.0 / (count + 1)) ** 0.5
    table = table.astype(np.float32)
    high = table.astype(jnp.bfloat16)
    low = (table - high.astype(np.float32)).astype(jnp.bfloat16)
    return high, low


def split(values):
    high = values.astype(BF16)
    low = (values - high.astype(F32)).astype(BF16)
    return high, low


def plan(chunks, packs):
    starts = [sum(chunks[:c]) for c in range(len(chunks))]
    early = min(EARLY, len(chunks))
    pieces = [(p, 1, starts[c], chunks[c]) for p in range(packs) for c in range(early)]
    pieces += [(0, packs, starts[c], chunks[c]) for c in range(early, len(chunks))]
    owner = list(range(early)) * packs + list(range(early, len(chunks)))
    return starts, early, pieces, owner


def kernel(
    north, deep, chunks,
    a_hbm, coupling_hbm, sym_x_hbm, sym_y_hbm, sym_z_hbm, tx_hbm, ty_hbm, tz_hbm,
    out,
    a, coupling, sym_x, sym_y, sym_z, tx, ty, tz, x1, r, s, t,
    given, r_given, s_given,
    load_sem, send_n, recv_n, send_d, recv_d, ready,
    send_lent, send_give, recv_give, send_pass, recv_pass, send_given,
):
    me_n = lax.axis_index("north")
    me_d = lax.axis_index("deep")
    fields, share_y, share_z, size_x = a.shape
    pack = LANES // share_z
    packs = fields // pack
    share_x = size_x // north
    size_y = share_y * north
    block_y = size_y // deep
    size_z = share_z * deep
    starts, early, pieces, owner = plan(chunks, packs)
    half = deep // 2
    last = len(pieces) - 1
    split_x = len(chunks) > LENT + 1
    first_x = starts[LENT] if split_x else 0
    sizes = chunks[LENT:LENT + 2] if split_x else [1, 1]
    shared = sum(sizes)
    upper, lower = me_d == half, me_d == half - 1
    inner, partner = upper | lower, deep - 1 - me_d
    lent = {owner.index(LENT): inner, owner.index(LENT + 1): upper} if split_x else {}
    odd = lax.rem(me_n, 2)

    loads = [pltpu.make_async_copy(tx_hbm, tx, load_sem.at[0])]
    for p in range(packs):
        part = pl.ds(p * pack, pack)
        loads.append(pltpu.make_async_copy(a_hbm.at[part], a.at[part], load_sem.at[1 + p]))
    pairs = [
        (ty_hbm, ty), (sym_x_hbm, sym_x), (sym_y_hbm, sym_y), (sym_z_hbm, sym_z),
        (coupling_hbm, coupling), (tz_hbm, tz),
    ]
    late = [
        pltpu.make_async_copy(source, target, load_sem.at[len(loads) + i])
        for i, (source, target) in enumerate(pairs)
    ]
    for copy in loads + late:
        copy.start()

    peers_n = [lax.rem(me_n + k, north) for k in range(1, north)]
    side = me_d // half
    across = [(1 - side) * half + j for j in range(half)]
    along = [side * half + lax.rem(me_d + j, half) for j in range(1, half)]
    peers_d = across + along

    barrier = pltpu.get_barrier_semaphore()
    for k in range(0, north, 2):
        even = lax.rem(me_n - odd + k, north)

        @pl.when(even != me_n)
        def _():
            pl.semaphore_signal(barrier, inc=1, device_id={"north": even}, device_id_type=MESH)

    @pl.when(odd == 0)
    def _():
        pl.semaphore_signal(barrier, inc=1, device_id={"north": me_n + 1}, device_id_type=MESH)

    for peer in peers_d:
        pl.semaphore_signal(
            barrier, inc=1, device_id={"north": me_n - odd + 1, "deep": peer}, device_id_type=MESH
        )

    def gather_north():
        pl.semaphore_wait(barrier, north - 1)
        pl.semaphore_signal(ready, inc=1, device_id={"north": me_n + 1}, device_id_type=MESH)

    def gather_deep():
        pl.semaphore_wait(barrier, 2 * (deep - 1) + 1)
        pl.semaphore_signal(ready, inc=1, device_id={"north": me_n - 1}, device_id_type=MESH)

    def be_ready():
        pl.semaphore_wait(ready, 1)

    def enter_north():
        pl.when(odd == 0)(gather_north)
        pl.when(odd == 1)(be_ready)

    def enter_deep():
        pl.when(odd == 1)(gather_deep)
        pl.when(odd == 0)(be_ready)

    def north_copy(c, peer):
        p, count, x, size = pieces[c]
        return pltpu.make_async_remote_copy(
            src_ref=x1.at[pl.ds(peer * share_x + x, size), pl.ds(p, count)],
            dst_ref=r.at[me_n, pl.ds(x, size), pl.ds(p, count)],
            send_sem=send_n,
            recv_sem=recv_n.at[c],
            device_id={"north": peer},
            device_id_type=MESH,
        )

    def deep_copy(c, peer):
        p, count, x, size = pieces[c]
        return pltpu.make_async_remote_copy(
            src_ref=s.at[peer, pl.ds(x, size), pl.ds(p, count)],
            dst_ref=t.at[me_d, pl.ds(x, size), pl.ds(p, count)],
            send_sem=send_lent.at[list(lent).index(c)] if c in lent else send_d,
            recv_sem=recv_d.at[owner[c]],
            device_id={"deep": peer},
            device_id_type=MESH,
        )

    def give(given_packs, size):
        for p in given_packs:
            for k in range(north):
                pltpu.make_async_remote_copy(
                    src_ref=x1.at[pl.ds(k * share_x + first_x, size), pl.ds(p, 1)],
                    dst_ref=given.at[k, pl.ds(0, size), pl.ds(p, 1)],
                    send_sem=send_give,
                    recv_sem=recv_give,
                    device_id={"deep": partner},
                    device_id_type=MESH,
                ).start()

    def enter_and_give(given_packs, size):
        enter_deep()
        give(given_packs, size)

    def pass_on(peer, size):
        return pltpu.make_async_remote_copy(
            src_ref=given.at[peer, pl.ds(0, size)],
            dst_ref=r_given.at[me_n, pl.ds(0, size)],
            send_sem=send_pass,
            recv_sem=recv_pass,
            device_id={"north": peer},
            device_id_type=MESH,
        )

    def take_and_pass(size):
        take(given.at[pl.ds(0, north), pl.ds(0, size)], recv_give)
        for peer in peers_n:
            pass_on(peer, size).start()
        r_given[me_n, 0:size] = given[me_n, 0:size]

    def transform_passed(size):
        take(r_given.at[pl.ds(0, north - 1), pl.ds(0, size)], recv_pass)
        to_modes(r_given, s_given, 0, packs, 0, size)
        x = 0
        for i in range(2 if size == shared else 1):
            part = pl.ds(x, sizes[i])
            place = t.at[partner, pl.ds(first_x + x, sizes[i])]
            arrival = recv_d.at[LENT + i]
            for peer in along:
                pltpu.make_async_remote_copy(
                    src_ref=s_given.at[peer, part],
                    dst_ref=place,
                    send_sem=send_given,
                    recv_sem=arrival,
                    device_id={"deep": peer},
                    device_id_type=MESH,
                ).start()
            pltpu.make_async_copy(s_given.at[me_d, part], place, arrival).start()
            x += sizes[i]

    def take(ref, sem):
        pltpu.make_async_copy(ref, ref, sem).wait()

    def north_arrived(c):
        p, count, x, size = pieces[c]
        take(r.at[pl.ds(0, north - 1), pl.ds(x, size), pl.ds(p, count)], recv_n.at[c])

    def deep_arrived(c):
        take(t.at[pl.ds(0, deep - 1), pl.ds(starts[c], chunks[c])], recv_d.at[c])

    def all_sent():
        take(r.at[pl.ds(0, north - 1)], send_n)
        if not split_x:
            take(t.at[pl.ds(0, deep - 1)], send_d)
            return
        take(t.at[pl.ds(0, deep - 1), pl.ds(0, share_x - shared)], send_d)

        def settle(gave, took, others):
            take(given.at[pl.ds(0, north), pl.ds(0, gave)], send_give)
            take(given.at[pl.ds(0, north - 1), pl.ds(0, took)], send_pass)
            if half > 1:
                take(s_given.at[pl.ds(0, half - 1), pl.ds(0, took)], send_given)
            for i, count in enumerate(others):
                if count:
                    take(t.at[pl.ds(0, count), pl.ds(0, sizes[i])], send_lent.at[i])

        @pl.when(upper)
        def _():
            settle(shared, sizes[0], [half - 1, half - 1])

        @pl.when(lower)
        def _():
            settle(sizes[0], shared, [half - 1, deep - 1])

        @pl.when(jnp.logical_not(inner))
        def _():
            for i in range(2):
                take(t.at[pl.ds(0, deep - 1), pl.ds(0, sizes[i])], send_lent.at[i])

    def to_modes(source, target, first, count, start, stop):
        for p in range(first, first + count):
            for x in range(start, stop, 2):
                width = min(2, stop - x)
                lines = [
                    jnp.concatenate([source[n, x + i, p] for n in range(north)], axis=0)
                    for i in range(width)
                ]
                high, low = split(jnp.concatenate(lines, axis=1))
                stack = jnp.concatenate([high, high, low], axis=0)
                mixed = jnp.dot(ty[...], stack, preferred_element_type=F32)
                for i in range(width):
                    modes = mixed[:, i * LANES:(i + 1) * LANES]
                    for d in range(deep):
                        target[d, x + i, p] = modes[d * block_y:(d + 1) * block_y]

    loads[0].wait()
    for p in range(packs):
        loads[1 + p].wait()
        for y in range(0, share_y, 2):
            rows = [a[p * pack + f, y + i] for i in range(2) for f in range(pack)]
            high, low = split(jnp.concatenate(rows, axis=0))
            lines = lax.dot_general(
                tx[...],
                jnp.concatenate([high, low], axis=1),
                dimension_numbers=(((1,), (1,)), ((), ())),
                preferred_element_type=F32,
            )
            lines = lines[:size_x] + lines[size_x:]
            x1[:, p, y, :] = lines[:, :LANES]
            x1[:, p, y + 1, :] = lines[:, LANES:]
        if p == 0:
            waits = me_n < north - 2
            if split_x:
                pl.when(upper & waits)(functools.partial(enter_and_give, [p], shared))
            enter_north()
        sent = range(p * early, (p + 1) * early if p < packs - 1 else len(pieces))
        for c in sent:
            for peer in peers_n:
                north_copy(c, peer).start()
        if split_x and p == 0:
            pl.when(upper & jnp.logical_not(waits))(functools.partial(enter_and_give, [p], shared))
        elif split_x:
            pl.when(upper)(functools.partial(give, [p], shared))
    if split_x:
        pl.when(lower)(functools.partial(enter_and_give, range(packs), sizes[0]))

    r[me_n] = x1[pl.ds(me_n * share_x, share_x)]

    for copy in late:
        copy.wait()

    rows_y = lax.broadcasted_iota(jnp.int32, (block_y, size_z), 0)
    base = jnp.broadcast_to(sym_z[...], (block_y, size_z))
    column = jnp.zeros((block_y, size_z), F32)
    for i in range(block_y):
        column = jnp.where(rows_y == i, sym_y[0, me_d * block_y + i], column)
    base = base + column

    for c in range(len(pieces)):
        first, count, start, size = pieces[c]
        if c == 0:
            if split_x:
                pl.when(jnp.logical_not(inner))(enter_deep)
            else:
                enter_deep()
        north_arrived(c)
        to_modes(r, s, first, count, start, start + size)
        crossing = [(c, peer, True) for peer in across[:-1]]
        beside = [(c, peer, False) for peer in along]
        now = crossing + beside if c == 0 else beside + crossing
        held = len(pieces) - min(HOLD, len(pieces))
        then = [c] if c < held else range(held, len(pieces)) if c == last else []
        for k, peer, crosses in now + [(k, across[-1], True) for k in then]:
            copy = deep_copy(k, peer)
            if k in lent and crosses:
                pl.when(jnp.logical_not(lent[k]))(copy.start)
            else:
                copy.start()

        if split_x and c == min(PASS, last):
            pl.when(lower)(functools.partial(take_and_pass, shared))

    if split_x:
        pl.when(upper)(functools.partial(take_and_pass, sizes[0]))
        pl.when(lower)(functools.partial(transform_passed, shared))
        pl.when(upper)(functools.partial(transform_passed, sizes[0]))

    t[me_d] = s[me_d]

    for c in range(len(chunks)):
        weights = []
        for x in range(starts[c], starts[c] + chunks[c]):
            weight = 1.0 / (1.0 + (base + sym_x[0, me_n * share_x + x]))
            weights.append((weight, 1.0 - weight))
        deep_arrived(c)
        height = chunks[c] * block_y
        rows = []
        for p in range(packs):
            lines = [
                t[d, starts[c]:starts[c] + chunks[c], p].reshape(height, LANES) for d in range(deep)
            ]
            for f in range(pack):
                rows.append(
                    jnp.concatenate(
                        [line[:, f * share_z:(f + 1) * share_z] for line in lines], axis=1
                    )
                )
        high, low = split(jnp.concatenate(rows, axis=0))
        main = jnp.dot(jnp.concatenate([high, low], axis=0), tz[0], preferred_element_type=F32)
        rest = jnp.dot(high, tz[1], preferred_element_type=F32)
        spectrum = main[:fields * height] + main[fields * height:] + rest
        for i in range(chunks[c]):
            x = starts[c] + i
            weight, other = weights[i]
            old = [
                spectrum[f * height + i * block_y:f * height + (i + 1) * block_y]
                for f in range(fields)
            ]
            for f in range(fields):
                total = coupling[f, 0] * old[0]
                for g in range(1, fields):
                    total = total + coupling[f, g] * old[g]
                out[f, x] = weight * old[f] + other * total

    all_sent()


def on_device(north, deep, velocity, coupling, symbol_x, symbol_y, symbol_z):
    field = jnp.transpose(velocity, (0, 2, 3, 1))
    fields, share_y, share_z, size_x = field.shape
    size_y, size_z = share_y * north, share_z * deep
    share_x, block_y = size_x // north, size_y // deep
    packs = fields * share_z // LANES
    unit = sum(SIZES)
    chunks = [size * share_x // unit for size in SIZES] if share_x % unit == 0 else [share_x]
    count = len(plan(chunks, packs)[2])
    lent = sum(chunks[LENT:LENT + 2]) if len(chunks) > LENT + 1 else 1
    high, low = basis_table(size_x)
    tx = jnp.asarray(np.block([[high, high], [low, np.zeros_like(low)]]))
    high, low = basis_table(size_y)
    ty = jnp.asarray(np.concatenate([high, low, high], axis=1))
    high, low = basis_table(size_z)
    tz = jnp.asarray(np.stack([high, low]))
    need = 4 * field.size * 8 + 2 * (tx.size + ty.size + tz.size) + 2**21
    vmem = pl.BlockSpec(memory_space=pltpu.VMEM)
    hbm = pl.BlockSpec(memory_space=pltpu.HBM)
    operands = (field, coupling, symbol_x[None, :], symbol_y[None, :], symbol_z[None, :], tx, ty, tz)
    return pl.pallas_call(
        functools.partial(kernel, north, deep, chunks),
        out_shape=jax.ShapeDtypeStruct((fields, share_x, block_y, size_z), F32),
        in_specs=[hbm] * 8,
        out_specs=vmem,
        scratch_shapes=[
            pltpu.VMEM(field.shape, F32),
            pltpu.SMEM(coupling.shape, F32),
            pltpu.SMEM((1, size_x), F32),
            pltpu.SMEM((1, size_y), F32),
            pltpu.VMEM((1, size_z), F32),
            pltpu.VMEM(tx.shape, BF16),
            pltpu.VMEM(ty.shape, BF16),
            pltpu.VMEM(tz.shape, BF16),
            pltpu.VMEM((size_x, packs, share_y, LANES), F32),
            pltpu.VMEM((north, share_x, packs, share_y, LANES), F32),
            pltpu.VMEM((deep, share_x, packs, block_y, LANES), F32),
            pltpu.VMEM((deep, share_x, packs, block_y, LANES), F32),
            pltpu.VMEM((north, lent, packs, share_y, LANES), F32),
            pltpu.VMEM((north, lent, packs, share_y, LANES), F32),
            pltpu.VMEM((deep, lent, packs, block_y, LANES), F32),
            pltpu.SemaphoreType.DMA((7 + packs,)),
            pltpu.SemaphoreType.DMA,
            pltpu.SemaphoreType.DMA((count,)),
            pltpu.SemaphoreType.DMA,
            pltpu.SemaphoreType.DMA((len(chunks),)),
            pltpu.SemaphoreType.REGULAR,
            pltpu.SemaphoreType.DMA((2,)),
            pltpu.SemaphoreType.DMA,
            pltpu.SemaphoreType.DMA,
            pltpu.SemaphoreType.DMA,
            pltpu.SemaphoreType.DMA,
            pltpu.SemaphoreType.DMA,
        ],
        compiler_params=pltpu.CompilerParams(
            collective_id=0, has_side_effects=True, vmem_limit_bytes=need
        ),
    )(*[pltpu.with_memory_space_constraint(v, pltpu.HBM) for v in operands])


def solution(mesh):
    placed = (P(None, None, "north", "deep"), P(), P(), P(), P())
    return jax.shard_map(
        functools.partial(on_device, mesh.shape["north"], mesh.shape["deep"]),
        mesh=mesh,
        in_specs=placed,
        out_specs=P(None, "north", "deep", None),
        check_vma=False,
    )
```

```python
import functools

import jax
import jax.numpy as jnp
import numpy as np
from jax import lax
from jax.experimental import pallas as pl
from jax.experimental.pallas import tpu as pltpu
from jax.sharding import PartitionSpec as P

LANES = 128
SIZES = (2, 2, 2, 2, 1, 2, 2, 1, 2)
HOLD = 5
PASS = 5
LENT = 3
F32 = jnp.float32
BF16 = jnp.bfloat16
MESH = pl.DeviceIdType.MESH


def basis_table(count):
    rank = np.arange(1, count + 1)
    turns = (rank[:, None] * rank[None, :]) % (2 * count + 2)
    table = np.sin(np.pi / (count + 1) * turns) * (2.0 / (count + 1)) ** 0.5
    table = table.astype(np.float32)
    high = table.astype(jnp.bfloat16)
    low = (table - high.astype(np.float32)).astype(jnp.bfloat16)
    return high, low


def split(values):
    high = values.astype(BF16)
    low = (values - high.astype(F32)).astype(BF16)
    return high, low


def plan(chunks, packs):
    starts = [sum(chunks[:c]) for c in range(len(chunks))]
    step = 1 if chunks[0] <= 4 else chunks[0]
    pieces = [(0, 1, x, step) for x in range(0, chunks[0], step)]
    pieces += [(p, 1, 0, chunks[0]) for p in range(1, packs)]
    early = len(pieces)
    pieces += [(0, packs, starts[c], chunks[c]) for c in range(1, len(chunks))]
    owner = [0] * early + list(range(1, len(chunks)))
    return starts, early, pieces, owner


def to_spectrum(t, tz, start, count, fields):
    deep, _, packs, block_y, _ = t.shape
    pack = fields // packs
    share_z = LANES // pack
    height = count * block_y
    rows = []
    for p in range(packs):
        lines = [t[d, start:start + count, p].reshape(height, LANES) for d in range(deep)]
        for f in range(pack):
            rows.append(
                jnp.concatenate([line[:, f * share_z:(f + 1) * share_z] for line in lines], axis=1)
            )
    high, low = split(jnp.concatenate(rows, axis=0))
    main = jnp.dot(jnp.concatenate([high, low], axis=0), tz[0], preferred_element_type=F32)
    rest = jnp.dot(high, tz[1], preferred_element_type=F32)
    whole = main[:fields * height] + main[fields * height:] + rest
    return [whole[f * height:(f + 1) * height] for f in range(fields)]


def finish(values, last_lines, last_weight, mixing, tz, out, tail, sem):
    fields, share_x, block_y, _ = values.shape
    count = last_weight.shape[0]
    first = share_x - count
    bulk = pltpu.make_async_copy(
        values.at[pl.ds(0, fields), pl.ds(0, first)], out.at[pl.ds(0, fields), pl.ds(0, first)],
        sem.at[0],
    )
    bulk.start()
    spectrum = to_spectrum(last_lines, tz, 0, count, fields)
    for i in range(count):
        for y in range(0, block_y, 8):
            weight = last_weight[i, y:y + 8]
            other = 1.0 - weight
            old = [value[i * block_y + y:i * block_y + y + 8] for value in spectrum]
            for f in range(fields):
                total = mixing[f, 0] * old[0]
                for g in range(1, fields):
                    total = total + mixing[f, g] * old[g]
                tail[f, i, y:y + 8] = weight * old[f] + other * total
    rest = pltpu.make_async_copy(
        tail, out.at[pl.ds(0, fields), pl.ds(first, count)], sem.at[1]
    )
    rest.start()
    bulk.wait()
    rest.wait()


def kernel(
    north, deep, chunks,
    a_hbm, coupling_hbm, sym_x_hbm, sym_y_hbm, sym_z_hbm, tx_hbm, ty_hbm, tz_hbm,
    out, last_lines, last_weight, mixing, tz,
    a, coupling, sym_x, sym_y, sym_z, tx, ty, x1, r, s, t,
    given, r_given, s_given,
    load_sem, send_n, recv_n, send_d, recv_d, ready,
    send_lent, send_give, recv_give, send_pass, recv_pass, send_given,
):
    me_n = lax.axis_index("north")
    me_d = lax.axis_index("deep")
    fields, share_y, share_z, size_x = a.shape
    pack = LANES // share_z
    packs = fields // pack
    share_x = size_x // north
    size_y = share_y * north
    block_y = size_y // deep
    size_z = share_z * deep
    starts, early, pieces, owner = plan(chunks, packs)
    half = deep // 2
    last = len(pieces) - 1
    split_x = len(chunks) > LENT + 1
    first_x = starts[LENT] if split_x else 0
    sizes = chunks[LENT:LENT + 2] if split_x else [1, 1]
    shared = sum(sizes)
    upper, lower = me_d == half, me_d == half - 1
    inner, partner = upper | lower, deep - 1 - me_d
    lent = {owner.index(LENT): inner, owner.index(LENT + 1): upper} if split_x else {}
    odd = lax.rem(me_n, 2)

    loads = [pltpu.make_async_copy(tx_hbm, tx, load_sem.at[0])]
    for p in range(packs):
        part = pl.ds(p * pack, pack)
        loads.append(pltpu.make_async_copy(a_hbm.at[part], a.at[part], load_sem.at[1 + p]))
    pairs = [
        (ty_hbm, ty), (sym_x_hbm, sym_x), (sym_y_hbm, sym_y), (sym_z_hbm, sym_z),
        (coupling_hbm, coupling), (tz_hbm, tz),
    ]
    late = [
        pltpu.make_async_copy(source, target, load_sem.at[len(loads) + i])
        for i, (source, target) in enumerate(pairs)
    ]
    for copy in loads + late:
        copy.start()

    peers_n = [lax.rem(me_n + k, north) for k in range(1, north)]
    side = me_d // half
    across = [(1 - side) * half + j for j in range(half)]
    along = [side * half + lax.rem(me_d + j, half) for j in range(1, half)]
    peers_d = across + along

    barrier = pltpu.get_barrier_semaphore()
    for k in range(0, north, 2):
        even = lax.rem(me_n - odd + k, north)

        @pl.when(even != me_n)
        def _():
            pl.semaphore_signal(barrier, inc=1, device_id={"north": even}, device_id_type=MESH)

    @pl.when(odd == 0)
    def _():
        pl.semaphore_signal(barrier, inc=1, device_id={"north": me_n + 1}, device_id_type=MESH)

    for peer in peers_d:
        pl.semaphore_signal(
            barrier, inc=1, device_id={"north": me_n - odd + 1, "deep": peer}, device_id_type=MESH
        )

    def gather_north():
        pl.semaphore_wait(barrier, north - 1)
        pl.semaphore_signal(ready, inc=1, device_id={"north": me_n + 1}, device_id_type=MESH)

    def gather_deep():
        pl.semaphore_wait(barrier, 2 * (deep - 1) + 1)
        pl.semaphore_signal(ready, inc=1, device_id={"north": me_n - 1}, device_id_type=MESH)

    def be_ready():
        pl.semaphore_wait(ready, 1)

    def enter_north():
        pl.when(odd == 0)(gather_north)
        pl.when(odd == 1)(be_ready)

    def enter_deep():
        pl.when(odd == 1)(gather_deep)
        pl.when(odd == 0)(be_ready)

    def north_copy(c, peer):
        p, count, x, size = pieces[c]
        return pltpu.make_async_remote_copy(
            src_ref=x1.at[pl.ds(peer * share_x + x, size), pl.ds(p, count)],
            dst_ref=r.at[me_n, pl.ds(x, size), pl.ds(p, count)],
            send_sem=send_n,
            recv_sem=recv_n.at[c],
            device_id={"north": peer},
            device_id_type=MESH,
        )

    def deep_copy(c, peer):
        p, count, x, size = pieces[c]
        return pltpu.make_async_remote_copy(
            src_ref=s.at[peer, pl.ds(x, size), pl.ds(p, count)],
            dst_ref=t.at[me_d, pl.ds(x, size), pl.ds(p, count)],
            send_sem=send_lent.at[list(lent).index(c)] if c in lent else send_d,
            recv_sem=recv_d.at[owner[c]],
            device_id={"deep": peer},
            device_id_type=MESH,
        )

    def give(given_packs, size):
        for p in given_packs:
            for k in range(north):
                pltpu.make_async_remote_copy(
                    src_ref=x1.at[pl.ds(k * share_x + first_x, size), pl.ds(p, 1)],
                    dst_ref=given.at[k, pl.ds(0, size), pl.ds(p, 1)],
                    send_sem=send_give,
                    recv_sem=recv_give,
                    device_id={"deep": partner},
                    device_id_type=MESH,
                ).start()

    def enter_and_give(given_packs, size):
        enter_deep()
        give(given_packs, size)

    def pass_on(peer, size):
        return pltpu.make_async_remote_copy(
            src_ref=given.at[peer, pl.ds(0, size)],
            dst_ref=r_given.at[me_n, pl.ds(0, size)],
            send_sem=send_pass,
            recv_sem=recv_pass,
            device_id={"north": peer},
            device_id_type=MESH,
        )

    def take_and_pass(size):
        take(given.at[pl.ds(0, north), pl.ds(0, size)], recv_give)
        for peer in peers_n:
            pass_on(peer, size).start()
        r_given[me_n, 0:size] = given[me_n, 0:size]

    def transform_passed(size):
        take(r_given.at[pl.ds(0, north - 1), pl.ds(0, size)], recv_pass)
        to_modes(r_given, s_given, 0, packs, 0, size)
        x = 0
        for i in range(2 if size == shared else 1):
            part = pl.ds(x, sizes[i])
            place = t.at[partner, pl.ds(first_x + x, sizes[i])]
            arrival = recv_d.at[LENT + i]
            for peer in along:
                pltpu.make_async_remote_copy(
                    src_ref=s_given.at[peer, part],
                    dst_ref=place,
                    send_sem=send_given,
                    recv_sem=arrival,
                    device_id={"deep": peer},
                    device_id_type=MESH,
                ).start()
            pltpu.make_async_copy(s_given.at[me_d, part], place, arrival).start()
            x += sizes[i]

    def take(ref, sem):
        pltpu.make_async_copy(ref, ref, sem).wait()

    def north_arrived(c):
        p, count, x, size = pieces[c]
        take(r.at[pl.ds(0, north - 1), pl.ds(x, size), pl.ds(p, count)], recv_n.at[c])

    def deep_arrived(c):
        take(t.at[pl.ds(0, deep - 1), pl.ds(starts[c], chunks[c])], recv_d.at[c])

    def all_sent():
        take(r.at[pl.ds(0, north - 1)], send_n)
        if not split_x:
            take(t.at[pl.ds(0, deep - 1)], send_d)
            return
        take(t.at[pl.ds(0, deep - 1), pl.ds(0, share_x - shared)], send_d)

        def settle(gave, took, others):
            take(given.at[pl.ds(0, north), pl.ds(0, gave)], send_give)
            take(given.at[pl.ds(0, north - 1), pl.ds(0, took)], send_pass)
            if half > 1:
                take(s_given.at[pl.ds(0, half - 1), pl.ds(0, took)], send_given)
            for i, count in enumerate(others):
                if count:
                    take(t.at[pl.ds(0, count), pl.ds(0, sizes[i])], send_lent.at[i])

        @pl.when(upper)
        def _():
            settle(shared, sizes[0], [half - 1, half - 1])

        @pl.when(lower)
        def _():
            settle(sizes[0], shared, [half - 1, deep - 1])

        @pl.when(jnp.logical_not(inner))
        def _():
            for i in range(2):
                take(t.at[pl.ds(0, deep - 1), pl.ds(0, sizes[i])], send_lent.at[i])

    def to_modes(source, target, first, count, start, stop):
        for p in range(first, first + count):
            for x in range(start, stop, 2):
                width = min(2, stop - x)
                lines = [
                    jnp.concatenate([source[n, x + i, p] for n in range(north)], axis=0)
                    for i in range(width)
                ]
                high, low = split(jnp.concatenate(lines, axis=1))
                stack = jnp.concatenate([high, high, low], axis=0)
                mixed = jnp.dot(ty[...], stack, preferred_element_type=F32)
                for i in range(width):
                    modes = mixed[:, i * LANES:(i + 1) * LANES]
                    for d in range(deep):
                        target[d, x + i, p] = modes[d * block_y:(d + 1) * block_y]

    loads[0].wait()
    for p in range(packs):
        loads[1 + p].wait()
        for y in range(0, share_y, 2):
            rows = [a[p * pack + f, y + i] for i in range(2) for f in range(pack)]
            high, low = split(jnp.concatenate(rows, axis=0))
            lines = lax.dot_general(
                tx[...],
                jnp.concatenate([high, low], axis=1),
                dimension_numbers=(((1,), (1,)), ((), ())),
                preferred_element_type=F32,
            )
            lines = lines[:size_x] + lines[size_x:]
            x1[:, p, y, :] = lines[:, :LANES]
            x1[:, p, y + 1, :] = lines[:, LANES:]
        if p == 0:
            waits = me_n < north - 2
            if split_x:
                pl.when(upper & waits)(functools.partial(enter_and_give, [p], shared))
            enter_north()
        sent = [c for c in range(early) if pieces[c][0] == p]
        sent += range(early, len(pieces)) if p == packs - 1 else []
        for c in sent:
            for peer in peers_n:
                north_copy(c, peer).start()
        if split_x and p == 0:
            pl.when(upper & jnp.logical_not(waits))(functools.partial(enter_and_give, [p], shared))
        elif split_x:
            pl.when(upper)(functools.partial(give, [p], shared))
    if split_x:
        pl.when(lower)(functools.partial(enter_and_give, range(packs), sizes[0]))

    r[me_n] = x1[pl.ds(me_n * share_x, share_x)]

    for copy in late:
        copy.wait()

    rows_y = lax.broadcasted_iota(jnp.int32, (block_y, size_z), 0)
    base = jnp.broadcast_to(sym_z[...], (block_y, size_z))
    column = jnp.zeros((block_y, size_z), F32)
    for i in range(block_y):
        column = jnp.where(rows_y == i, sym_y[0, me_d * block_y + i], column)
    base = base + column

    for c in range(len(pieces)):
        first, count, start, size = pieces[c]
        if c == 0:
            if split_x:
                pl.when(jnp.logical_not(inner))(enter_deep)
            else:
                enter_deep()
        north_arrived(c)
        to_modes(r, s, first, count, start, start + size)
        crossing = [(c, peer, True) for peer in across[:-1]]
        beside = [(c, peer, False) for peer in along]
        now = crossing + beside if c == 0 else beside + crossing
        held = len(pieces) - min(HOLD, len(pieces))
        then = [c] if c < held else range(held, len(pieces)) if c == last else []
        for k, peer, crosses in now + [(k, across[-1], True) for k in then]:
            copy = deep_copy(k, peer)
            if k in lent and crosses:
                pl.when(jnp.logical_not(lent[k]))(copy.start)
            else:
                copy.start()

        if split_x and c == min(PASS, last):
            pl.when(lower)(functools.partial(take_and_pass, shared))

    if split_x:
        pl.when(upper)(functools.partial(take_and_pass, sizes[0]))
        pl.when(lower)(functools.partial(transform_passed, shared))
        pl.when(upper)(functools.partial(transform_passed, sizes[0]))

    t[me_d] = s[me_d]

    for f in range(fields):
        for g in range(fields):
            mixing[f, g] = jnp.full((8, size_z), coupling[f, g], F32)

    for c in range(len(chunks)):
        weights = []
        for x in range(starts[c], starts[c] + chunks[c]):
            weight = 1.0 / (1.0 + (base + sym_x[0, me_n * share_x + x]))
            weights.append((weight, 1.0 - weight))
        deep_arrived(c)
        if c == len(chunks) - 1:
            last_lines[...] = t[:, starts[c]:starts[c] + chunks[c]]
            for i in range(chunks[c]):
                last_weight[i] = weights[i][0]
            continue
        spectrum = to_spectrum(t, tz, starts[c], chunks[c], fields)
        for i in range(chunks[c]):
            weight, other = weights[i]
            old = [value[i * block_y:(i + 1) * block_y] for value in spectrum]
            for f in range(fields):
                total = coupling[f, 0] * old[0]
                for g in range(1, fields):
                    total = total + coupling[f, g] * old[g]
                out[f, starts[c] + i] = weight * old[f] + other * total

    all_sent()


def on_device(north, deep, velocity, coupling, symbol_x, symbol_y, symbol_z):
    field = jnp.transpose(velocity, (0, 2, 3, 1))
    fields, share_y, share_z, size_x = field.shape
    size_y, size_z = share_y * north, share_z * deep
    share_x, block_y = size_x // north, size_y // deep
    packs = fields * share_z // LANES
    unit = sum(SIZES)
    chunks = [size * share_x // unit for size in SIZES] if share_x % unit == 0 else [share_x]
    count = len(plan(chunks, packs)[2])
    lent = sum(chunks[LENT:LENT + 2]) if len(chunks) > LENT + 1 else 1
    high, low = basis_table(size_x)
    tx = jnp.asarray(np.block([[high, high], [low, np.zeros_like(low)]]))
    high, low = basis_table(size_y)
    ty = jnp.asarray(np.concatenate([high, low, high], axis=1))
    high, low = basis_table(size_z)
    tz = jnp.asarray(np.stack([high, low]))
    need = 4 * field.size * 8 + 2 * (tx.size + ty.size + tz.size) + 2**21
    vmem = pl.BlockSpec(memory_space=pltpu.VMEM)
    hbm = pl.BlockSpec(memory_space=pltpu.HBM)
    operands = (field, coupling, symbol_x[None, :], symbol_y[None, :], symbol_z[None, :], tx, ty, tz)
    results = pl.pallas_call(
        functools.partial(kernel, north, deep, chunks),
        out_shape=[
            jax.ShapeDtypeStruct((fields, share_x, block_y, size_z), F32),
            jax.ShapeDtypeStruct((deep, chunks[-1], packs, block_y, LANES), F32),
            jax.ShapeDtypeStruct((chunks[-1], block_y, size_z), F32),
            jax.ShapeDtypeStruct((fields, fields, 8, size_z), F32),
            jax.ShapeDtypeStruct(tz.shape, BF16),
        ],
        in_specs=[hbm] * 8,
        out_specs=[vmem] * 5,
        scratch_shapes=[
            pltpu.VMEM(field.shape, F32),
            pltpu.SMEM(coupling.shape, F32),
            pltpu.SMEM((1, size_x), F32),
            pltpu.SMEM((1, size_y), F32),
            pltpu.VMEM((1, size_z), F32),
            pltpu.VMEM(tx.shape, BF16),
            pltpu.VMEM(ty.shape, BF16),
            pltpu.VMEM((size_x, packs, share_y, LANES), F32),
            pltpu.VMEM((north, share_x, packs, share_y, LANES), F32),
            pltpu.VMEM((deep, share_x, packs, block_y, LANES), F32),
            pltpu.VMEM((deep, share_x, packs, block_y, LANES), F32),
            pltpu.VMEM((north, lent, packs, share_y, LANES), F32),
            pltpu.VMEM((north, lent, packs, share_y, LANES), F32),
            pltpu.VMEM((deep, lent, packs, block_y, LANES), F32),
            pltpu.SemaphoreType.DMA((7 + packs,)),
            pltpu.SemaphoreType.DMA,
            pltpu.SemaphoreType.DMA((count,)),
            pltpu.SemaphoreType.DMA,
            pltpu.SemaphoreType.DMA((len(chunks),)),
            pltpu.SemaphoreType.REGULAR,
            pltpu.SemaphoreType.DMA((2,)),
            pltpu.SemaphoreType.DMA,
            pltpu.SemaphoreType.DMA,
            pltpu.SemaphoreType.DMA,
            pltpu.SemaphoreType.DMA,
            pltpu.SemaphoreType.DMA,
        ],
        compiler_params=pltpu.CompilerParams(
            collective_id=0, has_side_effects=True, vmem_limit_bytes=need
        ),
    )(*[pltpu.with_memory_space_constraint(v, pltpu.HBM) for v in operands])
    return pl.pallas_call(
        finish,
        out_shape=jax.ShapeDtypeStruct((fields, share_x, block_y, size_z), F32),
        in_specs=[vmem] * 5,
        out_specs=hbm,
        scratch_shapes=[
            pltpu.VMEM((fields, chunks[-1], block_y, size_z), F32),
            pltpu.SemaphoreType.DMA((2,)),
        ],
        compiler_params=pltpu.CompilerParams(vmem_limit_bytes=need),
    )(*results)


def solution(mesh):
    placed = (P(None, None, "north", "deep"), P(), P(), P(), P())
    return jax.shard_map(
        functools.partial(on_device, mesh.shape["north"], mesh.shape["deep"]),
        mesh=mesh,
        in_specs=placed,
        out_specs=P(None, "north", "deep", None),
        check_vma=False,
    )
```

```python
import functools

import jax
import jax.numpy as jnp
import numpy as np
from jax import lax
from jax.experimental import pallas as pl
from jax.experimental.pallas import tpu as pltpu
from jax.sharding import PartitionSpec as P

LANES = 128
SIZES = (2, 2, 2, 2, 1, 2, 2, 1, 2)
HOLD = 5
PASS = 5
LENT = 3
F32 = jnp.float32
BF16 = jnp.bfloat16
MESH = pl.DeviceIdType.MESH


def basis_table(count):
    rank = np.arange(1, count + 1)
    turns = (rank[:, None] * rank[None, :]) % (2 * count + 2)
    table = np.sin(np.pi / (count + 1) * turns) * (2.0 / (count + 1)) ** 0.5
    table = table.astype(np.float32)
    high = table.astype(jnp.bfloat16)
    low = (table - high.astype(np.float32)).astype(jnp.bfloat16)
    return high, low


def split(values):
    high = values.astype(BF16)
    low = (values - high.astype(F32)).astype(BF16)
    return high, low


def plan(chunks, packs):
    starts = [sum(chunks[:c]) for c in range(len(chunks))]
    step = 1 if chunks[0] <= 4 else chunks[0]
    pieces = [(0, 1, x, step) for x in range(0, chunks[0], step)]
    pieces += [(p, 1, 0, chunks[0]) for p in range(1, packs)]
    early = len(pieces)
    pieces += [(0, packs, starts[c], chunks[c]) for c in range(1, len(chunks))]
    owner = [0] * early + list(range(1, len(chunks)))
    return starts, early, pieces, owner


def to_spectrum(t, tz, start, count, fields):
    deep, _, packs, block_y, _ = t.shape
    pack = fields // packs
    share_z = LANES // pack
    height = count * block_y
    rows = []
    for p in range(packs):
        lines = [t[d, start:start + count, p].reshape(height, LANES) for d in range(deep)]
        for f in range(pack):
            rows.append(
                jnp.concatenate([line[:, f * share_z:(f + 1) * share_z] for line in lines], axis=1)
            )
    high, low = split(jnp.concatenate(rows, axis=0))
    main = jnp.dot(jnp.concatenate([high, low], axis=0), tz[0], preferred_element_type=F32)
    rest = jnp.dot(high, tz[1], preferred_element_type=F32)
    whole = main[:fields * height] + main[fields * height:] + rest
    return [whole[f * height:(f + 1) * height] for f in range(fields)]


def finish(values, last_lines, last_weight, mixing, tz, out, tail, sem):
    fields, share_x, block_y, _ = values.shape
    count = last_weight.shape[0]
    first = share_x - count
    bulk = pltpu.make_async_copy(
        values.at[pl.ds(0, fields), pl.ds(0, first)], out.at[pl.ds(0, fields), pl.ds(0, first)],
        sem.at[0],
    )
    bulk.start()
    spectrum = to_spectrum(last_lines, tz, 0, count, fields)
    for i in range(count):
        for y in range(0, block_y, 8):
            weight = last_weight[i, y:y + 8]
            other = 1.0 - weight
            old = [value[i * block_y + y:i * block_y + y + 8] for value in spectrum]
            for f in range(fields):
                total = mixing[f, 0] * old[0]
                for g in range(1, fields):
                    total = total + mixing[f, g] * old[g]
                tail[f, i, y:y + 8] = weight * old[f] + other * total
    rest = pltpu.make_async_copy(
        tail, out.at[pl.ds(0, fields), pl.ds(first, count)], sem.at[1]
    )
    rest.start()
    bulk.wait()
    rest.wait()


def kernel(
    north, deep, chunks,
    a_hbm, coupling_hbm, sym_x_hbm, sym_y_hbm, sym_z_hbm, tx_hbm, ty_hbm, tz_hbm,
    out, last_lines, last_weight, mixing, tz,
    a, coupling, sym_x, sym_y, sym_z, tx, ty, x1, r, s, t,
    given, r_given, s_given,
    load_sem, send_n, recv_n, send_d, recv_d, ready,
    send_lent, send_give, recv_give, send_pass, recv_pass, send_given,
):
    me_n = lax.axis_index("north")
    me_d = lax.axis_index("deep")
    fields, share_y, share_z, size_x = a.shape
    pack = LANES // share_z
    packs = fields // pack
    share_x = size_x // north
    size_y = share_y * north
    block_y = size_y // deep
    size_z = share_z * deep
    starts, early, pieces, owner = plan(chunks, packs)
    half = deep // 2
    last = len(pieces) - 1
    split_x = len(chunks) > LENT + 1
    first_x = starts[LENT] if split_x else 0
    sizes = chunks[LENT:LENT + 2] if split_x else [1, 1]
    shared = sum(sizes)
    upper, lower = me_d == half, me_d == half - 1
    inner, partner = upper | lower, deep - 1 - me_d
    lent = {owner.index(LENT): inner, owner.index(LENT + 1): upper} if split_x else {}
    odd = lax.rem(me_n, 2)

    loads = [pltpu.make_async_copy(tx_hbm, tx, load_sem.at[0])]
    for p in range(packs):
        part = pl.ds(p * pack, pack)
        loads.append(pltpu.make_async_copy(a_hbm.at[part], a.at[part], load_sem.at[1 + p]))
    pairs = [
        (ty_hbm, ty), (sym_x_hbm, sym_x), (sym_y_hbm, sym_y), (sym_z_hbm, sym_z),
        (coupling_hbm, coupling), (tz_hbm, tz),
    ]
    late = [
        pltpu.make_async_copy(source, target, load_sem.at[len(loads) + i])
        for i, (source, target) in enumerate(pairs)
    ]
    for copy in [loads[1], loads[0]]:
        copy.start()

    peers_n = [lax.rem(me_n + k, north) for k in range(1, north)]
    side = me_d // half
    across = [(1 - side) * half + j for j in range(half)]
    along = [side * half + lax.rem(me_d + j, half) for j in range(1, half)]
    peers_d = across + along

    barrier = pltpu.get_barrier_semaphore()
    for k in range(0, north, 2):
        even = lax.rem(me_n - odd + k, north)

        @pl.when(even != me_n)
        def _():
            pl.semaphore_signal(barrier, inc=1, device_id={"north": even}, device_id_type=MESH)

    @pl.when(odd == 0)
    def _():
        pl.semaphore_signal(barrier, inc=1, device_id={"north": me_n + 1}, device_id_type=MESH)

    for peer in peers_d:
        pl.semaphore_signal(
            barrier, inc=1, device_id={"north": me_n - odd + 1, "deep": peer}, device_id_type=MESH
        )

    def gather_north():
        pl.semaphore_wait(barrier, north - 1)
        pl.semaphore_signal(ready, inc=1, device_id={"north": me_n + 1}, device_id_type=MESH)

    def gather_deep():
        pl.semaphore_wait(barrier, 2 * (deep - 1) + 1)
        pl.semaphore_signal(ready, inc=1, device_id={"north": me_n - 1}, device_id_type=MESH)

    def be_ready():
        pl.semaphore_wait(ready, 1)

    def enter_north():
        pl.when(odd == 0)(gather_north)
        pl.when(odd == 1)(be_ready)

    def enter_deep():
        pl.when(odd == 1)(gather_deep)
        pl.when(odd == 0)(be_ready)

    def north_copy(c, peer):
        p, count, x, size = pieces[c]
        return pltpu.make_async_remote_copy(
            src_ref=x1.at[pl.ds(peer * share_x + x, size), pl.ds(p, count)],
            dst_ref=r.at[me_n, pl.ds(x, size), pl.ds(p, count)],
            send_sem=send_n,
            recv_sem=recv_n.at[c],
            device_id={"north": peer},
            device_id_type=MESH,
        )

    def deep_copy(c, peer):
        p, count, x, size = pieces[c]
        return pltpu.make_async_remote_copy(
            src_ref=s.at[peer, pl.ds(x, size), pl.ds(p, count)],
            dst_ref=t.at[me_d, pl.ds(x, size), pl.ds(p, count)],
            send_sem=send_lent.at[list(lent).index(c)] if c in lent else send_d,
            recv_sem=recv_d.at[owner[c]],
            device_id={"deep": peer},
            device_id_type=MESH,
        )

    def give(given_packs, size):
        for p in given_packs:
            for k in range(north):
                pltpu.make_async_remote_copy(
                    src_ref=x1.at[pl.ds(k * share_x + first_x, size), pl.ds(p, 1)],
                    dst_ref=given.at[k, pl.ds(0, size), pl.ds(p, 1)],
                    send_sem=send_give,
                    recv_sem=recv_give,
                    device_id={"deep": partner},
                    device_id_type=MESH,
                ).start()

    def enter_and_give(given_packs, size):
        enter_deep()
        give(given_packs, size)

    def pass_on(peer, size):
        return pltpu.make_async_remote_copy(
            src_ref=given.at[peer, pl.ds(0, size)],
            dst_ref=r_given.at[me_n, pl.ds(0, size)],
            send_sem=send_pass,
            recv_sem=recv_pass,
            device_id={"north": peer},
            device_id_type=MESH,
        )

    def take_and_pass(size):
        take(given.at[pl.ds(0, north), pl.ds(0, size)], recv_give)
        for peer in peers_n:
            pass_on(peer, size).start()
        r_given[me_n, 0:size] = given[me_n, 0:size]

    def transform_passed(size):
        take(r_given.at[pl.ds(0, north - 1), pl.ds(0, size)], recv_pass)
        to_modes(r_given, s_given, 0, packs, 0, size)
        x = 0
        for i in range(2 if size == shared else 1):
            part = pl.ds(x, sizes[i])
            place = t.at[partner, pl.ds(first_x + x, sizes[i])]
            arrival = recv_d.at[LENT + i]
            for peer in along:
                pltpu.make_async_remote_copy(
                    src_ref=s_given.at[peer, part],
                    dst_ref=place,
                    send_sem=send_given,
                    recv_sem=arrival,
                    device_id={"deep": peer},
                    device_id_type=MESH,
                ).start()
            pltpu.make_async_copy(s_given.at[me_d, part], place, arrival).start()
            x += sizes[i]

    def take(ref, sem):
        pltpu.make_async_copy(ref, ref, sem).wait()

    def north_arrived(c):
        p, count, x, size = pieces[c]
        take(r.at[pl.ds(0, north - 1), pl.ds(x, size), pl.ds(p, count)], recv_n.at[c])

    def deep_arrived(c):
        take(t.at[pl.ds(0, deep - 1), pl.ds(starts[c], chunks[c])], recv_d.at[c])

    def all_sent():
        take(r.at[pl.ds(0, north - 1)], send_n)
        if not split_x:
            take(t.at[pl.ds(0, deep - 1)], send_d)
            return
        take(t.at[pl.ds(0, deep - 1), pl.ds(0, share_x - shared)], send_d)

        def settle(gave, took, others):
            take(given.at[pl.ds(0, north), pl.ds(0, gave)], send_give)
            take(given.at[pl.ds(0, north - 1), pl.ds(0, took)], send_pass)
            if half > 1:
                take(s_given.at[pl.ds(0, half - 1), pl.ds(0, took)], send_given)
            for i, count in enumerate(others):
                if count:
                    take(t.at[pl.ds(0, count), pl.ds(0, sizes[i])], send_lent.at[i])

        @pl.when(upper)
        def _():
            settle(shared, sizes[0], [half - 1, half - 1])

        @pl.when(lower)
        def _():
            settle(sizes[0], shared, [half - 1, deep - 1])

        @pl.when(jnp.logical_not(inner))
        def _():
            for i in range(2):
                take(t.at[pl.ds(0, deep - 1), pl.ds(0, sizes[i])], send_lent.at[i])

    def to_modes(source, target, first, count, start, stop):
        for p in range(first, first + count):
            for x in range(start, stop, 2):
                width = min(2, stop - x)
                lines = [
                    jnp.concatenate([source[n, x + i, p] for n in range(north)], axis=0)
                    for i in range(width)
                ]
                high, low = split(jnp.concatenate(lines, axis=1))
                stack = jnp.concatenate([high, high, low], axis=0)
                mixed = jnp.dot(ty[...], stack, preferred_element_type=F32)
                for i in range(width):
                    modes = mixed[:, i * LANES:(i + 1) * LANES]
                    for d in range(deep):
                        target[d, x + i, p] = modes[d * block_y:(d + 1) * block_y]

    loads[0].wait()
    for p in range(packs):
        loads[1 + p].wait()
        for copy in loads[2:] + late if p == 0 else []:
            copy.start()
        for y in range(0, share_y, 2):
            rows = [a[p * pack + f, y + i] for i in range(2) for f in range(pack)]
            high, low = split(jnp.concatenate(rows, axis=0))
            lines = lax.dot_general(
                tx[...],
                jnp.concatenate([high, low], axis=1),
                dimension_numbers=(((1,), (1,)), ((), ())),
                preferred_element_type=F32,
            )
            lines = lines[:size_x] + lines[size_x:]
            x1[:, p, y, :] = lines[:, :LANES]
            x1[:, p, y + 1, :] = lines[:, LANES:]
        if p == 0:
            waits = me_n < north - 2
            if split_x:
                pl.when(upper & waits)(functools.partial(enter_and_give, [p], shared))
            enter_north()
        sent = [c for c in range(early) if pieces[c][0] == p]
        sent += range(early, len(pieces)) if p == packs - 1 else []
        for c in sent:
            for peer in peers_n:
                north_copy(c, peer).start()
        if split_x and p == 0:
            pl.when(upper & jnp.logical_not(waits))(functools.partial(enter_and_give, [p], shared))
        elif split_x:
            pl.when(upper)(functools.partial(give, [p], shared))
    if split_x:
        pl.when(lower)(functools.partial(enter_and_give, range(packs), sizes[0]))

    r[me_n] = x1[pl.ds(me_n * share_x, share_x)]

    for copy in late:
        copy.wait()

    rows_y = lax.broadcasted_iota(jnp.int32, (block_y, size_z), 0)
    base = jnp.broadcast_to(sym_z[...], (block_y, size_z))
    column = jnp.zeros((block_y, size_z), F32)
    for i in range(block_y):
        column = jnp.where(rows_y == i, sym_y[0, me_d * block_y + i], column)
    base = base + column

    for c in range(len(pieces)):
        first, count, start, size = pieces[c]
        if c == 0:
            if split_x:
                pl.when(jnp.logical_not(inner))(enter_deep)
            else:
                enter_deep()
        north_arrived(c)
        to_modes(r, s, first, count, start, start + size)
        crossing = [(c, peer, True) for peer in across[:-1]]
        beside = [(c, peer, False) for peer in along]
        now = crossing + beside if c == 0 else beside + crossing
        held = len(pieces) - min(HOLD, len(pieces))
        then = [c] if c < held else range(held, len(pieces)) if c == last else []
        for k, peer, crosses in now + [(k, across[-1], True) for k in then]:
            copy = deep_copy(k, peer)
            if k in lent and crosses:
                pl.when(jnp.logical_not(lent[k]))(copy.start)
            else:
                copy.start()

        if split_x and c == min(PASS, last):
            pl.when(lower)(functools.partial(take_and_pass, shared))

    if split_x:
        pl.when(upper)(functools.partial(take_and_pass, sizes[0]))
        pl.when(lower)(functools.partial(transform_passed, shared))
        pl.when(upper)(functools.partial(transform_passed, sizes[0]))

    t[me_d] = s[me_d]

    for f in range(fields):
        for g in range(fields):
            mixing[f, g] = jnp.full((8, size_z), coupling[f, g], F32)

    for c in range(len(chunks)):
        weights = []
        for x in range(starts[c], starts[c] + chunks[c]):
            weight = 1.0 / (1.0 + (base + sym_x[0, me_n * share_x + x]))
            weights.append((weight, 1.0 - weight))
        deep_arrived(c)
        if c == len(chunks) - 1:
            last_lines[...] = t[:, starts[c]:starts[c] + chunks[c]]
            for i in range(chunks[c]):
                last_weight[i] = weights[i][0]
            continue
        spectrum = to_spectrum(t, tz, starts[c], chunks[c], fields)
        for i in range(chunks[c]):
            weight, other = weights[i]
            old = [value[i * block_y:(i + 1) * block_y] for value in spectrum]
            for f in range(fields):
                total = coupling[f, 0] * old[0]
                for g in range(1, fields):
                    total = total + coupling[f, g] * old[g]
                out[f, starts[c] + i] = weight * old[f] + other * total

    all_sent()


def on_device(north, deep, velocity, coupling, symbol_x, symbol_y, symbol_z):
    field = jnp.transpose(velocity, (0, 2, 3, 1))
    fields, share_y, share_z, size_x = field.shape
    size_y, size_z = share_y * north, share_z * deep
    share_x, block_y = size_x // north, size_y // deep
    packs = fields * share_z // LANES
    unit = sum(SIZES)
    chunks = [size * share_x // unit for size in SIZES] if share_x % unit == 0 else [share_x]
    count = len(plan(chunks, packs)[2])
    lent = sum(chunks[LENT:LENT + 2]) if len(chunks) > LENT + 1 else 1
    high, low = basis_table(size_x)
    tx = jnp.asarray(np.block([[high, high], [low, np.zeros_like(low)]]))
    high, low = basis_table(size_y)
    ty = jnp.asarray(np.concatenate([high, low, high], axis=1))
    high, low = basis_table(size_z)
    tz = jnp.asarray(np.stack([high, low]))
    need = 4 * field.size * 8 + 2 * (tx.size + ty.size + tz.size) + 2**21
    vmem = pl.BlockSpec(memory_space=pltpu.VMEM)
    hbm = pl.BlockSpec(memory_space=pltpu.HBM)
    operands = (field, coupling, symbol_x[None, :], symbol_y[None, :], symbol_z[None, :], tx, ty, tz)
    results = pl.pallas_call(
        functools.partial(kernel, north, deep, chunks),
        out_shape=[
            jax.ShapeDtypeStruct((fields, share_x, block_y, size_z), F32),
            jax.ShapeDtypeStruct((deep, chunks[-1], packs, block_y, LANES), F32),
            jax.ShapeDtypeStruct((chunks[-1], block_y, size_z), F32),
            jax.ShapeDtypeStruct((fields, fields, 8, size_z), F32),
            jax.ShapeDtypeStruct(tz.shape, BF16),
        ],
        in_specs=[hbm] * 8,
        out_specs=[vmem] * 5,
        scratch_shapes=[
            pltpu.VMEM(field.shape, F32),
            pltpu.SMEM(coupling.shape, F32),
            pltpu.SMEM((1, size_x), F32),
            pltpu.SMEM((1, size_y), F32),
            pltpu.VMEM((1, size_z), F32),
            pltpu.VMEM(tx.shape, BF16),
            pltpu.VMEM(ty.shape, BF16),
            pltpu.VMEM((size_x, packs, share_y, LANES), F32),
            pltpu.VMEM((north, share_x, packs, share_y, LANES), F32),
            pltpu.VMEM((deep, share_x, packs, block_y, LANES), F32),
            pltpu.VMEM((deep, share_x, packs, block_y, LANES), F32),
            pltpu.VMEM((north, lent, packs, share_y, LANES), F32),
            pltpu.VMEM((north, lent, packs, share_y, LANES), F32),
            pltpu.VMEM((deep, lent, packs, block_y, LANES), F32),
            pltpu.SemaphoreType.DMA((7 + packs,)),
            pltpu.SemaphoreType.DMA,
            pltpu.SemaphoreType.DMA((count,)),
            pltpu.SemaphoreType.DMA,
            pltpu.SemaphoreType.DMA((len(chunks),)),
            pltpu.SemaphoreType.REGULAR,
            pltpu.SemaphoreType.DMA((2,)),
            pltpu.SemaphoreType.DMA,
            pltpu.SemaphoreType.DMA,
            pltpu.SemaphoreType.DMA,
            pltpu.SemaphoreType.DMA,
            pltpu.SemaphoreType.DMA,
        ],
        compiler_params=pltpu.CompilerParams(
            collective_id=0, has_side_effects=True, vmem_limit_bytes=need
        ),
    )(*[pltpu.with_memory_space_constraint(v, pltpu.HBM) for v in operands])
    return pl.pallas_call(
        finish,
        out_shape=jax.ShapeDtypeStruct((fields, share_x, block_y, size_z), F32),
        in_specs=[vmem] * 5,
        out_specs=hbm,
        scratch_shapes=[
            pltpu.VMEM((fields, chunks[-1], block_y, size_z), F32),
            pltpu.SemaphoreType.DMA((2,)),
        ],
        compiler_params=pltpu.CompilerParams(vmem_limit_bytes=need),
    )(*results)


def solution(mesh):
    placed = (P(None, None, "north", "deep"), P(), P(), P(), P())
    return jax.shard_map(
        functools.partial(on_device, mesh.shape["north"], mesh.shape["deep"]),
        mesh=mesh,
        in_specs=placed,
        out_specs=P(None, "north", "deep", None),
        check_vma=False,
    )
```
